32 devices in a mesh: sys: 1 (over z), row: 32 (over y, x, core).
Axes of the slice: x: 4, y: 4, z: 1, core: 2. Of those that a mesh axis runs over, the one named last changes fastest.
The devices are a block of a 4x4x8 slice.
Arguments:
- positions: bfloat16 [32768, 128], P(('sys', 'row'))
- charges: float32 [32768], P(('sys', 'row'))
- counts: int32 [32], P(('sys', 'row'))
Outputs:
- output 1: float32 [32768, 128], P(('sys', 'row'))
- output 2: float32 [1], P('sys')
All inputs are finite; a program needn't handle non-finite values.
Results may differ from the reference program's by a relative error of at most 0.001.
Values are sent between devices in bfloat16 or wider.
A program may use at most 768 MiB of HBM per device.

```python
import jax
import jax.numpy as jnp
from jax import lax

BLOCK_ROWS = 1024
D = 128
RING_SIZE = 32
NUM_ROWS = RING_SIZE * BLOCK_ROWS
ROW_TILE = min(BLOCK_ROWS, 256)


def setup_inputs(seed: int = 0, part: int = 0) -> dict:
    part_key = jax.random.fold_in(jax.random.key(seed), part)
    sub_keys = jax.random.split(part_key, 6)
    positions = jax.random.normal(sub_keys[0], (NUM_ROWS, D), jnp.float32).astype(jnp.bfloat16)
    sign_vals = jnp.where(jax.random.bernoulli(sub_keys[1], 0.5, (NUM_ROWS,)), 1.0, -1.0)
    magnitude = jax.random.uniform(sub_keys[2], (NUM_ROWS,), jnp.float32, 0.5, 1.5)
    charges = (sign_vals * magnitude).astype(jnp.float32)
    counts = jax.random.randint(sub_keys[3], (RING_SIZE,), BLOCK_ROWS // 16, BLOCK_ROWS + 1)
    full_slot = jax.random.randint(sub_keys[4], (), 0, RING_SIZE)
    small_slot = (full_slot + jax.random.randint(sub_keys[5], (), 1, RING_SIZE)) % RING_SIZE
    counts = counts.at[full_slot].set(BLOCK_ROWS).at[small_slot].set(BLOCK_ROWS // 16)
    return {'positions': positions, 'charges': charges, 'counts': counts.astype(jnp.int32)}


def reference(positions, charges, counts):
    is_valid = jnp.arange(BLOCK_ROWS)[None, :] < counts[:, None]
    live_q = jnp.where(is_valid, charges.reshape(RING_SIZE, BLOCK_ROWS), 0.0).reshape(NUM_ROWS)
    pos_f32 = positions.astype(jnp.float32)
    sq_norm = jnp.sum(pos_f32 * pos_f32, axis=1)
    col_ids = jnp.arange(NUM_ROWS)
    neg_scale = -0.5 / D
    inv_len2 = 1.0 / D

    def tile_terms(tile_idx):
        row_start = tile_idx * ROW_TILE
        row_block = lax.dynamic_slice(positions, (row_start, 0), (ROW_TILE, D))
        row_q = lax.dynamic_slice(live_q, (row_start,), (ROW_TILE,))
        row_sq = lax.dynamic_slice(sq_norm, (row_start,), (ROW_TILE,))
        gram_mat = jnp.dot(row_block, positions.T, preferred_element_type=jnp.float32)
        dist_sq = jnp.maximum(row_sq[:, None] + sq_norm[None, :] - 2.0 * gram_mat, 0.0)
        weight = row_q[:, None] * live_q[None, :] * jnp.exp(dist_sq * neg_scale)
        row_ids = row_start + jnp.arange(ROW_TILE)
        weight = jnp.where(row_ids[:, None] == col_ids[None, :], 0.0, weight)
        pulled = jnp.dot(weight.astype(jnp.bfloat16), positions, preferred_element_type=jnp.float32)
        row_force = (jnp.sum(weight, axis=1)[:, None] * row_block.astype(jnp.float32) - pulled) * inv_len2
        return row_force, jnp.sum(weight)

    tile_forces, tile_energy = lax.map(tile_terms, jnp.arange(NUM_ROWS // ROW_TILE))
    return tile_forces.reshape(NUM_ROWS, D), (0.5 * jnp.sum(tile_energy)).reshape(1)
```

```python
import functools
import math

import jax
import jax.numpy as jnp
from jax import lax
from jax.experimental import pallas as pl
from jax.experimental.pallas import tpu as pltpu
from jax.sharding import PartitionSpec as P

MESH = pl.DeviceIdType.MESH
BF16, F32 = jnp.bfloat16, jnp.float32
TILE = 256
AUG = 16
S_CAP = 1.69e38
C_CAP = 3.3895313892515355e38


def split3(val):
    hi = jnp.clip(val, -C_CAP, C_CAP).astype(BF16).astype(F32)
    mid = (val - hi).astype(BF16).astype(F32)
    low = (val - hi - mid).astype(BF16).astype(F32)
    return hi, mid, low


def dot(lhs, rhs, dims):
    return lax.dot_general(lhs, rhs, (dims, ((), ())), preferred_element_type=F32)


def stage_list(side):
    far = side // 2
    assert side == 4
    return [(0, 1), (0, -1), (1, 0), (-1, 0), (0, far), (1, 1), (1, -1), (-1, 1), (-1, -1), (far, 0),
            (1, far), (-1, far), (far, 1), (far, -1), (far, far)]


def kernel(side, width, x_ref, q_ref, cnt_ref, out_ref, e_ref, slots, xa, ci, s_acc, t_acc, ebuf,
           send_sem, recv_sem, dsend_sem, drecv_sem, esend_sem, erecv_sem):
    rows = x_ref.shape[0]
    n_tiles = rows // TILE
    half = n_tiles // 2
    n_dev = 2 * side * side
    me = lax.axis_index('row')
    sys_id = lax.axis_index('sys')
    core = lax.rem(me, 2)
    chip = lax.div(me, 2)
    pos_y, pos_x = lax.div(chip, side), lax.rem(chip, side)
    stages = stage_list(side)
    scale = math.log2(math.e) / width

    def dev(dy, dx, plane):
        return (lax.rem(pos_y + dy + side, side) * side + lax.rem(pos_x + dx + side, side)) * 2 + plane

    mate = me + 1 - 2 * core
    barrier = pltpu.get_barrier_semaphore()

    def greet(step, carry):
        pl.semaphore_signal(barrier, inc=1, device_id=(sys_id, lax.rem(me + step, n_dev)), device_id_type=MESH)
        return carry
    lax.fori_loop(1, n_dev, greet, 0)

    count = cnt_ref[0]
    row_id = lax.broadcasted_iota(jnp.int32, (rows, width), 0)
    lane_id = lax.broadcasted_iota(jnp.int32, (rows, width), 1)
    x_val = jnp.where(row_id < count, x_ref[...].astype(F32), 0.0)
    x_t = x_val.T
    s_row = -jnp.minimum(0.5 * jnp.sum(x_t * x_t, axis=0, keepdims=True), S_CAP)
    s_col = -jnp.minimum(0.5 * jnp.sum(x_val * x_val, axis=1, keepdims=True), S_CAP)
    q_shape = q_ref.shape
    q_id = lax.broadcasted_iota(jnp.int32, q_shape, 0) * q_shape[1] + lax.broadcasted_iota(jnp.int32, q_shape, 1)
    q_val = jnp.where(q_id < count, q_ref[...], 0.0)
    q_row = jnp.concatenate([q_val[r:r + 1, :] for r in range(q_shape[0])], axis=1)
    aug_id = lax.broadcasted_iota(jnp.int32, (AUG, rows), 0)
    aug = jnp.where(aug_id < 3, 1.0, 0.0)
    for k, part in enumerate(split3(s_row) + split3(q_row)):
        aug = jnp.where(aug_id == 3 + k, part, aug)
    for t in range(n_tiles):
        cols = slice(t * TILE, (t + 1) * TILE)
        slots[me * n_tiles + t, :width, :] = x_t[:, cols].astype(BF16)
        slots[me * n_tiles + t, width:, :] = aug[:, cols].astype(BF16)
    xa[:, :width] = x_val.astype(BF16)
    tail = jnp.where((lane_id >= 3) & (lane_id < 6), 1.0, 0.0)
    for k, part in enumerate(split3(s_col)):
        tail = jnp.where(lane_id == k, part, tail)
    xa[:, width:] = tail.astype(BF16)
    q_t = q_val.T
    for r in range(q_shape[0]):
        lanes = q_shape[1]
        ci[r * lanes:(r + 1) * lanes, :] = jnp.broadcast_to(q_t[:, r:r + 1], (lanes, width))
    s_acc[...] = jnp.zeros_like(s_acc)
    t_acc[...] = jnp.zeros_like(t_acc)

    pl.semaphore_wait(barrier, n_dev - 1)

    def wrap(d):
        return (d + 1) % side - 1
    stage_of = {d: k for k, d in enumerate(stages)}
    sends = []

    def stage_disp(k, t):
        dy, dx = stages[k]
        return (dy, dx) if t < half else (dx, dy)

    def make_send(disp, t, hop, idx):
        dy, dx = wrap(disp[0] - hop[0]), wrap(disp[1] - hop[1])
        k = stage_of[(dy, dx) if t < half else (dx, dy)]
        unit = dev(disp[0], disp[1], core) * n_tiles + t
        return pltpu.make_async_remote_copy(
            src_ref=slots.at[unit], dst_ref=slots.at[unit], send_sem=send_sem.at[idx], recv_sem=recv_sem.at[k, t],
            device_id=(sys_id, dev(hop[0], hop[1], core)), device_id_type=MESH)

    def flip(pair, t):
        return pair if t < half else (pair[1], pair[0])

    def relays(k):
        found = []
        slow, fast = (0, 0) if k < 0 else stages[k]
        for t in range(n_tiles):
            first = t % half == 0
            if k < 0:
                found += [((0, 0), t, flip((0, sgn), t)) for sgn in (1, -1)]
            elif slow == 0 and abs(fast) == 1 and first == (fast == 1):
                found.append((flip((slow, fast), t), t, flip((0, -fast), t)))
        for t in range(n_tiles):
            first = t % half == 0
            if slow == 0:
                found += [(flip((slow, fast), t), t, flip((sgn, 0), t)) for sgn in (1, -1)]
            elif abs(slow) == 1 and first == (slow == 1):
                found.append((flip((slow, fast), t), t, flip((-slow, 0), t)))
        return found

    def start_relays(k):
        for disp, t, hop in relays(k):
            make_send(disp, t, hop, len(sends)).start()
            sends.append(0)

    def mate_copy(k, part):
        dy, dx = (0, 0) if k < 0 else stage_disp(k, part * half)
        unit = dev(dy, dx, core) * n_tiles + part * half
        return pltpu.make_async_remote_copy(
            src_ref=slots.at[pl.ds(unit, half)], dst_ref=slots.at[pl.ds(unit, half)],
            send_sem=dsend_sem.at[k + 1, part], recv_sem=drecv_sem.at[k + 1, part],
            device_id=(sys_id, mate), device_id_type=MESH)

    def mate_recv(k, part):
        dy, dx = (0, 0) if k < 0 else stage_disp(k, part * half)
        unit = dev(dy, dx, 1 - core) * n_tiles + part * half
        return pltpu.make_async_remote_copy(
            src_ref=slots.at[pl.ds(unit, half)], dst_ref=slots.at[pl.ds(unit, half)],
            send_sem=dsend_sem.at[k + 1, part], recv_sem=drecv_sem.at[k + 1, part],
            device_id=(sys_id, mate), device_id_type=MESH)

    def recv(k, t):
        dy, dx = stage_disp(k, t)
        unit = dev(dy, dx, core) * n_tiles + t
        return pltpu.make_async_remote_copy(
            src_ref=slots.at[unit], dst_ref=slots.at[unit], send_sem=send_sem.at[0], recv_sem=recv_sem.at[k, t],
            device_id=(sys_id, mate), device_id_type=MESH)

    eye = (lax.broadcasted_iota(jnp.int32, (TILE, TILE), 0) == lax.broadcasted_iota(jnp.int32, (TILE, TILE), 1))
    pad = jnp.zeros((2 * width - width - AUG, TILE), BF16)

    def column_tile(unit, diag=None):
        block = slots[unit]
        aug_rhs = jnp.concatenate([block, pad], axis=0)
        parts = block[width:, :].astype(F32)
        cj = parts[6:7, :] + parts[7:8, :] + parts[8:9, :]
        for it in range(n_tiles):
            mine = slice(it * TILE, (it + 1) * TILE)
            arg = dot(xa[mine, :], aug_rhs, ((1,), (0,)))
            weight = jnp.exp2(jnp.minimum(arg, 0.0) * scale) * cj
            if it == diag:
                weight = jnp.where(eye, 0.0, weight)
            c_mine = ci[mine, :]
            left, right = weight[:, :width] * c_mine, weight[:, width:] * c_mine
            s_acc[mine, :] += left + right
            w_low = jnp.concatenate([left, right], axis=1).astype(BF16)
            t_acc[mine, :] += dot(w_low, block[:width, :], ((1,), (1,)))

    start_relays(-1)
    for part in range(2):
        mate_copy(-1, part).start()
    for t in range(n_tiles):
        column_tile(me * n_tiles + t, diag=t)

    def base_unit(step, part, plane):
        dy, dx = jnp.int32(0), jnp.int32(0)
        for k in range(len(stages)):
            sy, sx = stage_disp(k, part * half)
            dy = jnp.where(step == k, sy, dy)
            dx = jnp.where(step == k, sx, dx)
        return dev(dy, dx, plane) * n_tiles + part * half

    def step_body(step, carry):
        for k in range(len(stages)):
            @pl.when(step == k)
            def _():
                for t in range(n_tiles):
                    recv(k, t).wait_recv()
                start_relays(k)
                for part in range(2):
                    mate_copy(k, part).start()
                for part in range(2):
                    mate_recv(k - 1, part).wait_recv()
        for part in range(2):
            unit = base_unit(step, part, core)
            for t in range(half):
                column_tile(unit + t)
        for part in range(2):
            unit = base_unit(step - 1, part, 1 - core)
            for t in range(half):
                column_tile(unit + t)
        return carry
    lax.fori_loop(0, len(stages), step_body, 0)
    last = len(stages) - 1
    for part in range(2):
        mate_recv(last, part).wait_recv()
    for part in range(2):
        unit = base_unit(last, part, 1 - core)
        for t in range(half):
            column_tile(unit + t)

    s_sum = jnp.sum(s_acc[...], axis=1, keepdims=True)
    x_own = xa[:, :width].astype(F32)
    out_ref[...] = (s_sum * x_own - t_acc[...]) * (1.0 / width)
    ebuf[me] = jnp.sum(s_acc[...].reshape(rows // 8, 8, width), axis=0)

    def e_copy(step):
        return pltpu.make_async_remote_copy(
            src_ref=ebuf.at[me], dst_ref=ebuf.at[me], send_sem=esend_sem.at[step], recv_sem=erecv_sem.at[me],
            device_id=(sys_id, lax.rem(me + step, n_dev)), device_id_type=MESH)

    def e_start(step, carry):
        e_copy(step).start()
        return carry
    lax.fori_loop(1, n_dev, e_start, 0)

    def e_wait(step, carry):
        src = lax.rem(me + step, n_dev)
        pltpu.make_async_remote_copy(
            src_ref=ebuf.at[src], dst_ref=ebuf.at[src], send_sem=esend_sem.at[step], recv_sem=erecv_sem.at[src],
            device_id=(sys_id, mate), device_id_type=MESH).wait_recv()
        return carry
    lax.fori_loop(1, n_dev, e_wait, 0)
    e_ref[0] = 0.5 * jnp.sum(ebuf[...])

    def e_sent(step, carry):
        e_copy(step).wait_send()
        return carry
    lax.fori_loop(1, n_dev, e_sent, 0)

    def sent(idx, carry):
        pltpu.make_async_remote_copy(
            src_ref=slots.at[0], dst_ref=slots.at[0], send_sem=send_sem.at[idx], recv_sem=recv_sem.at[0, 0],
            device_id=(sys_id, mate), device_id_type=MESH).wait_send()
        return carry
    lax.fori_loop(0, len(sends), sent, 0)
    for k in range(-1, len(stages)):
        for part in range(2):
            mate_copy(k, part).wait_send()


def solution(mesh):
    n_dev = mesh.shape['row']
    side = math.isqrt(n_dev // 2)

    def per_device(positions, charges, counts):
        rows, width = positions.shape
        n_tiles = rows // TILE
        n_stages = len(stage_list(side))
        n_sends = n_tiles * n_stages
        vmem = pl.BlockSpec(memory_space=pltpu.VMEM)
        smem = pl.BlockSpec(memory_space=pltpu.SMEM)
        force, energy = pl.pallas_call(
            functools.partial(kernel, side, width),
            out_shape=[jax.ShapeDtypeStruct((rows, width), F32), jax.ShapeDtypeStruct((1,), F32)],
            in_specs=[vmem, vmem, smem],
            out_specs=[vmem, smem],
            scratch_shapes=[
                pltpu.VMEM((n_dev * n_tiles, width + AUG, TILE), BF16),
                pltpu.VMEM((rows, 2 * width), BF16),
                pltpu.VMEM((rows, width), F32),
                pltpu.VMEM((rows, width), F32),
                pltpu.VMEM((rows, width), F32),
                pltpu.VMEM((n_dev, 8, width), F32),
                pltpu.SemaphoreType.DMA((n_sends,)),
                pltpu.SemaphoreType.DMA((n_stages, n_tiles)),
                pltpu.SemaphoreType.DMA((n_stages + 1, 2)),
                pltpu.SemaphoreType.DMA((n_stages + 1, 2)),
                pltpu.SemaphoreType.DMA((n_dev,)),
                pltpu.SemaphoreType.DMA((n_dev,)),
            ],
            compiler_params=pltpu.CompilerParams(collective_id=0, has_side_effects=True, vmem_limit_bytes=48 * 2 ** 20),
            name='pair_forces',
        )(positions, charges.reshape(rows // width, width), counts)
        return force, energy

    row_spec = P(('sys', 'row'), None)
    vec_spec = P(('sys', 'row'))
    return jax.shard_map(per_device, mesh=mesh, in_specs=(row_spec, vec_spec, vec_spec),
                         out_specs=(row_spec, P('sys')), check_vma=False)
```

```python
import functools
import math

import jax
import jax.numpy as jnp
from jax import lax
from jax.experimental import pallas as pl
from jax.experimental.pallas import tpu as pltpu
from jax.sharding import PartitionSpec as P

MESH = pl.DeviceIdType.MESH
BF16, F32 = jnp.bfloat16, jnp.float32
TILE = 256
AUG = 16
S_CAP = 1.69e38
C_CAP = 3.3895313892515355e38


def split3(val):
    hi = jnp.clip(val, -C_CAP, C_CAP).astype(BF16).astype(F32)
    mid = (val - hi).astype(BF16).astype(F32)
    low = (val - hi - mid).astype(BF16).astype(F32)
    return hi, mid, low


def dot(lhs, rhs, dims):
    return lax.dot_general(lhs, rhs, (dims, ((), ())), preferred_element_type=F32)


def stage_list(side):
    far = side // 2
    assert side == 4
    return [(0, 1), (0, -1), (1, 0), (-1, 0), (0, far), (1, 1), (1, -1), (-1, 1), (-1, -1), (far, 0),
            (1, far), (-1, far), (far, 1), (far, -1), (far, far)]


ARRIVALS = {-1: (0,), 0: (1,), 1: (2,), 2: (3,), 3: (4,), 4: (5, 6), 5: (7, 8), 6: (10, 11), 7: (9,), 8: (12,), 9: (14, 13)}
COMPUTE = (0, 1, 2, 3, 4, 5, 6, 7, 10, 9, 12, 14, 8, 11, 13)
SHARE = (1.0, 0.0, 1.0, 0.0, 0.5, 1.0, 0.5, 0.5, 0.0, 0.5, 1.0, 0.0, 1.0, 0.0, 0.5)
ENERGY_STEP = 12


def kernel(side, width, x_hbm, q_hbm, cnt_ref, out_ref, e_ref, x_ref, q_ref, in_sem, slots, xa, ci, s_acc, t_acc, ebuf,
           send_sem, recv_sem, dsend_sem, drecv_sem, esend_sem, erecv_sem):
    x_in = pltpu.make_async_copy(x_hbm, x_ref, in_sem.at[0])
    q_in = pltpu.make_async_copy(q_hbm, q_ref, in_sem.at[1])
    x_in.start()
    q_in.start()
    rows = x_ref.shape[0]
    n_tiles = rows // TILE
    half = n_tiles // 2
    n_dev = 2 * side * side
    me = lax.axis_index('row')
    sys_id = lax.axis_index('sys')
    core = lax.rem(me, 2)
    chip = lax.div(me, 2)
    pos_y, pos_x = lax.div(chip, side), lax.rem(chip, side)
    stages = stage_list(side)
    scale = math.log2(math.e) / width

    def dev(dy, dx, plane):
        return (lax.rem(pos_y + dy + side, side) * side + lax.rem(pos_x + dx + side, side)) * 2 + plane

    mate = me + 1 - 2 * core
    barrier = pltpu.get_barrier_semaphore()

    near = [dev(0, 1, core), dev(0, -1, core), dev(1, 0, core), dev(-1, 0, core), mate]
    for peer in near:
        pl.semaphore_signal(barrier, inc=1, device_id=(sys_id, peer), device_id_type=MESH)
    x_in.wait()
    q_in.wait()

    count = cnt_ref[0]
    row_id = lax.broadcasted_iota(jnp.int32, (rows, width), 0)
    lane_id = lax.broadcasted_iota(jnp.int32, (rows, width), 1)
    x_val = jnp.where(row_id < count, x_ref[...].astype(F32), 0.0)
    x_t = x_val.T
    s_row = -jnp.minimum(0.5 * jnp.sum(x_t * x_t, axis=0, keepdims=True), S_CAP)
    s_col = -jnp.minimum(0.5 * jnp.sum(x_val * x_val, axis=1, keepdims=True), S_CAP)
    q_shape = q_ref.shape
    q_id = lax.broadcasted_iota(jnp.int32, q_shape, 0) * q_shape[1] + lax.broadcasted_iota(jnp.int32, q_shape, 1)
    q_val = jnp.where(q_id < count, q_ref[...], 0.0)
    q_row = jnp.concatenate([q_val[r:r + 1, :] for r in range(q_shape[0])], axis=1)
    aug_id = lax.broadcasted_iota(jnp.int32, (AUG, rows), 0)
    aug = jnp.where(aug_id < 3, 1.0, 0.0)
    for k, part in enumerate(split3(s_row) + split3(q_row)):
        aug = jnp.where(aug_id == 3 + k, part, aug)
    for t in range(n_tiles):
        cols = slice(t * TILE, (t + 1) * TILE)
        slots[me * n_tiles + t, :width, :] = x_t[:, cols].astype(BF16)
        slots[me * n_tiles + t, width:, :] = aug[:, cols].astype(BF16)
    xa[:, :width] = x_val.astype(BF16)
    tail = jnp.where((lane_id >= 3) & (lane_id < 6), 1.0, 0.0)
    for k, part in enumerate(split3(s_col)):
        tail = jnp.where(lane_id == k, part, tail)
    xa[:, width:] = tail.astype(BF16)
    q_t = q_val.T
    for r in range(q_shape[0]):
        lanes = q_shape[1]
        ci[r * lanes:(r + 1) * lanes, :] = jnp.broadcast_to(q_t[:, r:r + 1], (lanes, width))
    s_acc[...] = jnp.zeros_like(s_acc)
    t_acc[...] = jnp.zeros_like(t_acc)

    pl.semaphore_wait(barrier, len(near))

    def wrap(d):
        return (d + 1) % side - 1
    stage_of = {d: k for k, d in enumerate(stages)}
    sends = []

    def stage_disp(k, t):
        dy, dx = stages[k]
        return (dy, dx) if t < half else (dx, dy)

    def make_send(disp, t, hop, idx):
        dy, dx = wrap(disp[0] - hop[0]), wrap(disp[1] - hop[1])
        k = stage_of[(dy, dx) if t < half else (dx, dy)]
        unit = dev(disp[0], disp[1], core) * n_tiles + t
        return pltpu.make_async_remote_copy(
            src_ref=slots.at[unit], dst_ref=slots.at[unit], send_sem=send_sem.at[idx], recv_sem=recv_sem.at[k, t],
            device_id=(sys_id, dev(hop[0], hop[1], core)), device_id_type=MESH)

    def flip(pair, t):
        return pair if t < half else (pair[1], pair[0])

    def relays(k):
        found = []
        slow, fast = (0, 0) if k < 0 else stages[k]
        for t in range(n_tiles):
            first = t % half == 0
            if k < 0:
                found += [((0, 0), t, flip((0, sgn), t)) for sgn in (1, -1)]
            elif slow == 0 and abs(fast) == 1 and first == (fast == 1):
                found.append((flip((slow, fast), t), t, flip((0, -fast), t)))
        for t in range(n_tiles):
            first = t % half == 0
            if slow == 0:
                found += [(flip((slow, fast), t), t, flip((sgn, 0), t)) for sgn in (1, -1)]
            elif abs(slow) == 1 and first == (slow == 1):
                found.append((flip((slow, fast), t), t, flip((-slow, 0), t)))
        return found

    def start_relays(k):
        for disp, t, hop in relays(k):
            make_send(disp, t, hop, len(sends)).start()
            sends.append(0)

    def mate_copy(k, part):
        dy, dx = (0, 0) if k < 0 else stage_disp(k, part * half)
        unit = dev(dy, dx, core) * n_tiles + part * half
        return pltpu.make_async_remote_copy(
            src_ref=slots.at[pl.ds(unit, half)], dst_ref=slots.at[pl.ds(unit, half)],
            send_sem=dsend_sem.at[k + 1, part], recv_sem=drecv_sem.at[k + 1, part],
            device_id=(sys_id, mate), device_id_type=MESH)

    def mate_recv(k, part):
        dy, dx = (0, 0) if k < 0 else stage_disp(k, part * half)
        unit = dev(dy, dx, 1 - core) * n_tiles + part * half
        return pltpu.make_async_remote_copy(
            src_ref=slots.at[pl.ds(unit, half)], dst_ref=slots.at[pl.ds(unit, half)],
            send_sem=dsend_sem.at[k + 1, part], recv_sem=drecv_sem.at[k + 1, part],
            device_id=(sys_id, mate), device_id_type=MESH)

    def recv(k, t):
        dy, dx = stage_disp(k, t)
        unit = dev(dy, dx, core) * n_tiles + t
        return pltpu.make_async_remote_copy(
            src_ref=slots.at[unit], dst_ref=slots.at[unit], send_sem=send_sem.at[0], recv_sem=recv_sem.at[k, t],
            device_id=(sys_id, mate), device_id_type=MESH)

    eye = (lax.broadcasted_iota(jnp.int32, (TILE, TILE), 0) == lax.broadcasted_iota(jnp.int32, (TILE, TILE), 1))
    pad = jnp.zeros((2 * width - width - AUG, TILE), BF16)

    def column_tile(unit, diag=None):
        block = slots[unit]
        aug_rhs = jnp.concatenate([block, pad], axis=0)
        parts = block[width:, :].astype(F32)
        cj = parts[6:7, :] + parts[7:8, :] + parts[8:9, :]
        for it in range(n_tiles):
            mine = slice(it * TILE, (it + 1) * TILE)
            arg = dot(xa[mine, :], aug_rhs, ((1,), (0,)))
            weight = jnp.exp2(jnp.minimum(arg, 0.0) * scale) * cj
            if it == diag:
                weight = jnp.where(eye, 0.0, weight)
            c_mine = ci[mine, :]
            left, right = weight[:, :width] * c_mine, weight[:, width:] * c_mine
            s_acc[mine, :] += left + right
            w_low = jnp.concatenate([left, right], axis=1).astype(BF16)
            t_acc[mine, :] += dot(w_low, block[:width, :], ((1,), (1,)))

    start_relays(-1)
    for part in range(2):
        mate_copy(-1, part).start()
    for t in range(n_tiles):
        column_tile(me * n_tiles + t, diag=t)

    def base_unit(step, part, plane):
        dy, dx = jnp.int32(0), jnp.int32(0)
        for now in range(len(stages)):
            sy, sx = stage_disp(COMPUTE[now], part * half)
            dy = jnp.where(step == now, sy, dy)
            dx = jnp.where(step == now, sx, dx)
        return dev(dy, dx, plane) * n_tiles + part * half

    def arrive(k):
        for t in range(n_tiles):
            recv(k, t).wait_recv()
        start_relays(k)
        for part in range(2):
            mate_copy(k, part).start()

    def e_copy(step):
        return pltpu.make_async_remote_copy(
            src_ref=ebuf.at[me], dst_ref=ebuf.at[me], send_sem=esend_sem.at[step], recv_sem=erecv_sem.at[me],
            device_id=(sys_id, lax.rem(me + step, n_dev)), device_id_type=MESH)

    def e_start(step, carry):
        e_copy(step).start()
        return carry

    def tally(weight):
        ebuf[me] += weight * jnp.sum(s_acc[...].reshape(rows // 8, 8, width), axis=0)

    arrive(ARRIVALS[-1][0])
    for part in range(2):
        mate_recv(-1, part).wait_recv()
    ebuf[me] = jnp.zeros(ebuf.shape[1:], F32)
    for t in range(n_tiles):
        column_tile((mate * n_tiles) + t)
    share = [0.5] + [SHARE[k] for k in COMPUTE]

    def step_body(step, carry):
        for now in range(len(stages)):
            @pl.when(step == now)
            def _():
                for k in ARRIVALS.get(now, ()):
                    arrive(k)
                for part in range(2):
                    mate_recv(COMPUTE[now], part).wait_recv()
                if now <= ENERGY_STEP and share[now] != share[now + 1]:
                    tally(share[now] - share[now + 1])
                if now == ENERGY_STEP:
                    lax.fori_loop(1, n_dev, e_start, 0)
        for part in range(2):
            for plane in (core, 1 - core):
                unit = base_unit(step, part, plane)
                for t in range(half):
                    column_tile(unit + t)
        return carry
    lax.fori_loop(0, len(stages), step_body, 0)

    s_sum = jnp.sum(s_acc[...], axis=1, keepdims=True)
    x_own = xa[:, :width].astype(F32)
    out_ref[...] = (s_sum * x_own - t_acc[...]) * (1.0 / width)
    def e_wait(step, carry):
        src = lax.rem(me + step, n_dev)
        pltpu.make_async_remote_copy(
            src_ref=ebuf.at[src], dst_ref=ebuf.at[src], send_sem=esend_sem.at[step], recv_sem=erecv_sem.at[src],
            device_id=(sys_id, mate), device_id_type=MESH).wait_recv()
        return carry
    lax.fori_loop(1, n_dev, e_wait, 0)
    e_ref[0] = jnp.sum(ebuf[...])

    def e_sent(step, carry):
        e_copy(step).wait_send()
        return carry
    lax.fori_loop(1, n_dev, e_sent, 0)

    def sent(idx, carry):
        pltpu.make_async_remote_copy(
            src_ref=slots.at[0], dst_ref=slots.at[0], send_sem=send_sem.at[idx], recv_sem=recv_sem.at[0, 0],
            device_id=(sys_id, mate), device_id_type=MESH).wait_send()
        return carry
    lax.fori_loop(0, len(sends), sent, 0)
    for k in range(-1, len(stages)):
        for part in range(2):
            mate_copy(k, part).wait_send()


def solution(mesh):
    n_dev = mesh.shape['row']
    side = math.isqrt(n_dev // 2)

    def per_device(positions, charges, counts):
        rows, width = positions.shape
        n_tiles = rows // TILE
        n_stages = len(stage_list(side))
        n_sends = n_tiles * n_stages
        vmem = pl.BlockSpec(memory_space=pltpu.VMEM)
        smem = pl.BlockSpec(memory_space=pltpu.SMEM)
        hbm = pl.BlockSpec(memory_space=pl.ANY)
        force, energy = pl.pallas_call(
            functools.partial(kernel, side, width),
            out_shape=[jax.ShapeDtypeStruct((rows, width), F32), jax.ShapeDtypeStruct((1,), F32)],
            in_specs=[hbm, hbm, smem],
            out_specs=[vmem, smem],
            scratch_shapes=[
                pltpu.VMEM((rows, width), BF16),
                pltpu.VMEM((rows // width, width), F32),
                pltpu.SemaphoreType.DMA((2,)),
                pltpu.VMEM((n_dev * n_tiles, width + AUG, TILE), BF16),
                pltpu.VMEM((rows, 2 * width), BF16),
                pltpu.VMEM((rows, width), F32),
                pltpu.VMEM((rows, width), F32),
                pltpu.VMEM((rows, width), F32),
                pltpu.VMEM((n_dev, 8, width), F32),
                pltpu.SemaphoreType.DMA((n_sends,)),
                pltpu.SemaphoreType.DMA((n_stages, n_tiles)),
                pltpu.SemaphoreType.DMA((n_stages + 1, 2)),
                pltpu.SemaphoreType.DMA((n_stages + 1, 2)),
                pltpu.SemaphoreType.DMA((n_dev,)),
                pltpu.SemaphoreType.DMA((n_dev,)),
            ],
            compiler_params=pltpu.CompilerParams(collective_id=0, has_side_effects=True, vmem_limit_bytes=48 * 2 ** 20),
            name='pair_forces',
        )(positions, charges.reshape(rows // width, width), counts)
        return force, energy

    row_spec = P(('sys', 'row'), None)
    vec_spec = P(('sys', 'row'))
    return jax.shard_map(per_device, mesh=mesh, in_specs=(row_spec, vec_spec, vec_spec),
                         out_specs=(row_spec, P('sys')), check_vma=False)
```

```python
import functools
import math

import jax
import jax.numpy as jnp
from jax import lax
from jax.experimental import pallas as pl
from jax.experimental.pallas import tpu as pltpu
from jax.sharding import PartitionSpec as P

MESH = pl.DeviceIdType.MESH
BF16, F32 = jnp.bfloat16, jnp.float32
TILE = 256
AUG = 16
S_CAP = 1.69e38
C_CAP = 3.3895313892515355e38

SIDE, TILES = 4, 4
PAIRS = [(0, 2), (1, 1), (1, -1), (-1, 1), (-1, -1), (2, 0), (1, 2), (-1, 2), (2, 1), (2, -1), (2, 2)]
STAGES = [[((0, 1), t), ((0, -1), t), ((1, 0), t + 2), ((-1, 0), t + 2)] for t in (0, 1)]
STAGES += [[((1, 0), t), ((-1, 0), t), ((0, 1), t + 2), ((0, -1), t + 2)] for t in (0, 1)]
STAGES += [[((a, b), 0), ((a, b), 1), ((b, a), 2), ((b, a), 3)] for a, b in PAIRS]
STAGE_OF = {piece: (k, j) for k, stage in enumerate(STAGES) for j, piece in enumerate(stage)}
SHARE = (0.5, 0.5, 0.5, 0.5, 0.5, 1.0, 0.5, 0.5, 0.0, 0.5, 1.0, 0.0, 1.0, 0.0, 0.5)
COMPUTE = (0, 1, 2, 3, 4, 5, 6, 7, 10, 9, 12, 14, 8, 11, 13)
ARRIVALS = {0: (1,), 1: (2,), 2: (3,), 3: (4,), 4: (5, 6), 5: (7, 8), 6: (10, 11), 7: (9,), 8: (12,), 9: (14, 13)}
ENERGY_AT = 12


def wrap(d):
    return (d + 1) % SIDE - 1


def relays(piece):
    (slow, fast), t = piece
    swap = t >= TILES // 2
    if swap:
        slow, fast = fast, slow
    lead = 1 if t % 2 == 0 else -1
    hops = []
    if slow == 0 and fast == 0:
        hops += [(0, 1), (0, -1)]
    elif slow == 0 and fast == lead:
        hops += [(0, -fast)]
    if slow == 0:
        hops += [(1, 0), (-1, 0)]
    elif slow == lead:
        hops += [(-slow, 0)]
    return [(b, a) if swap else (a, b) for a, b in hops]


def relay_list(k):
    pieces = [((0, 0), t) for t in range(TILES)] if k < 0 else STAGES[k]
    found = []
    for piece in pieces:
        swap = piece[1] >= TILES // 2
        for hop in relays(piece):
            along = hop[1] if not swap else hop[0]
            found.append((0 if along else 1, len(found), piece, hop))
    return [(piece, hop) for _, _, piece, hop in sorted(found)]


def dot(lhs, rhs, dims):
    return lax.dot_general(lhs, rhs, (dims, ((), ())), preferred_element_type=F32)


def split3(val):
    hi = jnp.clip(val, -C_CAP, C_CAP).astype(BF16).astype(F32)
    mid = (val - hi).astype(BF16).astype(F32)
    low = (val - hi - mid).astype(BF16).astype(F32)
    return hi, mid, low


def kernel(width, x_hbm, q_hbm, cnt_ref, out_ref, e_ref, x_ref, q_ref, in_sem, slots, xa, ci, s_acc, t_acc, ebuf,
           send_sem, recv_sem, dsend_sem, drecv_sem, esend_sem, erecv_sem):
    rows = x_ref.shape[0]
    n_dev = 2 * SIDE * SIDE
    n_steps = len(STAGES)
    me = lax.axis_index('row')
    sys_id = lax.axis_index('sys')
    core = lax.rem(me, 2)
    chip = lax.div(me, 2)
    pos_y, pos_x = lax.div(chip, SIDE), lax.rem(chip, SIDE)
    mate = me + 1 - 2 * core
    scale = math.log2(math.e) / width

    def dev(dy, dx, plane):
        return (lax.rem(pos_y + dy + SIDE, SIDE) * SIDE + lax.rem(pos_x + dx + SIDE, SIDE)) * 2 + plane

    x_in = pltpu.make_async_copy(x_hbm, x_ref, in_sem.at[0])
    q_in = pltpu.make_async_copy(q_hbm, q_ref, in_sem.at[1])
    x_in.start()
    q_in.start()
    barrier = pltpu.get_barrier_semaphore()
    near = [dev(0, 1, core), dev(0, -1, core), dev(1, 0, core), dev(-1, 0, core), mate]
    for peer in near:
        pl.semaphore_signal(barrier, inc=1, device_id=(sys_id, peer), device_id_type=MESH)
    s_acc[...] = jnp.zeros_like(s_acc)
    t_acc[...] = jnp.zeros_like(t_acc)
    x_in.wait()
    q_in.wait()

    count = cnt_ref[0]
    row_id = lax.broadcasted_iota(jnp.int32, (rows, width), 0)
    lane_id = lax.broadcasted_iota(jnp.int32, (rows, width), 1)
    x_val = jnp.where(row_id < count, x_ref[...].astype(F32), 0.0)
    x_t = x_val.T
    s_row = -jnp.minimum(0.5 * jnp.sum(x_t * x_t, axis=0, keepdims=True), S_CAP)
    q_shape = q_ref.shape
    q_id = lax.broadcasted_iota(jnp.int32, q_shape, 0) * q_shape[1] + lax.broadcasted_iota(jnp.int32, q_shape, 1)
    q_val = jnp.where(q_id < count, q_ref[...], 0.0)
    q_row = jnp.concatenate([q_val[r:r + 1, :] for r in range(q_shape[0])], axis=1)
    aug_id = lax.broadcasted_iota(jnp.int32, (AUG, rows), 0)
    aug = jnp.where(aug_id < 3, 1.0, 0.0)
    for k, part in enumerate(split3(s_row) + split3(q_row)):
        aug = jnp.where(aug_id == 3 + k, part, aug)
    for t in range(TILES):
        cols = slice(t * TILE, (t + 1) * TILE)
        slots[me * TILES + t, :width, :] = x_t[:, cols].astype(BF16)
        slots[me * TILES + t, width:, :] = aug[:, cols].astype(BF16)
    pl.semaphore_wait(barrier, len(near))

    sends = []

    def unit_of(piece, plane):
        return dev(piece[0][0], piece[0][1], plane) * TILES + piece[1]

    def remote(unit, send, recv, peer):
        return pltpu.make_async_remote_copy(src_ref=slots.at[unit], dst_ref=slots.at[unit], send_sem=send, recv_sem=recv,
                                            device_id=(sys_id, peer), device_id_type=MESH)

    def start_relays(k):
        for piece, hop in relay_list(k):
            there = ((wrap(piece[0][0] - hop[0]), wrap(piece[0][1] - hop[1])), piece[1])
            remote(unit_of(piece, core), send_sem.at[len(sends)], recv_sem.at[STAGE_OF[there]],
                   dev(hop[0], hop[1], core)).start()
            sends.append(k)

    def pieces(k):
        return [((0, 0), t) for t in range(TILES)] if k < 0 else STAGES[k]

    def to_mate(k, j, plane):
        return remote(unit_of(pieces(k)[j], plane), dsend_sem.at[k + 1, j], drecv_sem.at[k + 1, j], mate)

    def arrive(k):
        for j in range(TILES):
            remote(unit_of(STAGES[k][j], core), send_sem.at[0], recv_sem.at[k, j], mate).wait_recv()
        start_relays(k)
        for j in range(TILES):
            to_mate(k, j, core).start()

    def from_mate(k):
        for j in range(TILES):
            to_mate(k, j, 1 - core).wait_recv()

    start_relays(-1)
    for j in range(TILES):
        to_mate(-1, j, core).start()

    s_col = -jnp.minimum(0.5 * jnp.sum(x_val * x_val, axis=1, keepdims=True), S_CAP)
    xa[:, :width] = x_val.astype(BF16)
    tail = jnp.where((lane_id >= 3) & (lane_id < 6), 1.0, 0.0)
    for k, part in enumerate(split3(s_col)):
        tail = jnp.where(lane_id == k, part, tail)
    xa[:, width:] = tail.astype(BF16)
    q_t = q_val.T
    for r in range(q_shape[0]):
        lanes = q_shape[1]
        ci[r * lanes:(r + 1) * lanes, :] = jnp.broadcast_to(q_t[:, r:r + 1], (lanes, width))

    eye = (lax.broadcasted_iota(jnp.int32, (TILE, TILE), 0) == lax.broadcasted_iota(jnp.int32, (TILE, TILE), 1))
    pad = jnp.zeros((width - AUG, TILE), BF16)

    def column_tile(unit, diag=None):
        block = slots[unit]
        rhs = jnp.concatenate([block, pad], axis=0)
        parts = block[width:, :].astype(F32)
        c_cols = parts[6:7, :] + parts[7:8, :] + parts[8:9, :]
        for it in range(rows // TILE):
            mine = slice(it * TILE, (it + 1) * TILE)
            arg = dot(xa[mine, :], rhs, ((1,), (0,)))
            weight = jnp.exp2(jnp.minimum(arg, 0.0) * scale) * c_cols
            if it == diag:
                weight = jnp.where(eye, 0.0, weight)
            c_mine = ci[mine, :]
            left, right = weight[:, :width] * c_mine, weight[:, width:] * c_mine
            s_acc[mine, :] += left + right
            w_low = jnp.concatenate([left, right], axis=1).astype(BF16)
            t_acc[mine, :] += dot(w_low, block[:width, :], ((1,), (1,)))

    for t in range(TILES):
        column_tile(me * TILES + t, diag=t)
    arrive(0)
    from_mate(-1)
    for t in range(TILES):
        column_tile(mate * TILES + t)
    ebuf[me] = jnp.zeros(ebuf.shape[1:], F32)

    def e_copy(step):
        return pltpu.make_async_remote_copy(
            src_ref=ebuf.at[me], dst_ref=ebuf.at[me], send_sem=esend_sem.at[step], recv_sem=erecv_sem.at[me],
            device_id=(sys_id, lax.rem(me + step, n_dev)), device_id_type=MESH)

    def e_start(step, carry):
        e_copy(step).start()
        return carry

    def tally(weight):
        ebuf[me] += weight * jnp.sum(s_acc[...].reshape(rows // 8, 8, width), axis=0)

    share = [0.5] + [SHARE[k] for k in COMPUTE]

    def step_units(step):
        units = []
        for j in range(TILES):
            code = jnp.int32(0)
            for now, k in enumerate(COMPUTE):
                (dy, dx), t = STAGES[k][j]
                code = jnp.where(step == now, ((dy % SIDE) * SIDE + dx % SIDE) * TILES + t, code)
            for plane in (core, 1 - core):
                units.append(dev(lax.div(code, SIDE * TILES), lax.rem(lax.div(code, TILES), SIDE), plane) * TILES
                             + lax.rem(code, TILES))
        return units

    def step_body(step, carry):
        for now in range(n_steps):
            @pl.when(step == now)
            def _():
                for k in ARRIVALS.get(now, ()):
                    arrive(k)
                from_mate(COMPUTE[now])
                if now <= ENERGY_AT and share[now] != share[now + 1]:
                    tally(share[now] - share[now + 1])
                if now == ENERGY_AT:
                    lax.fori_loop(1, n_dev, e_start, 0)
        for unit in step_units(step):
            column_tile(unit)
        return carry
    lax.fori_loop(0, n_steps, step_body, 0)

    s_sum = jnp.sum(s_acc[...], axis=1, keepdims=True)
    out_ref[...] = (s_sum * xa[:, :width].astype(F32) - t_acc[...]) * (1.0 / width)

    def e_wait(step, carry):
        src = lax.rem(me + step, n_dev)
        pltpu.make_async_remote_copy(
            src_ref=ebuf.at[src], dst_ref=ebuf.at[src], send_sem=esend_sem.at[step], recv_sem=erecv_sem.at[src],
            device_id=(sys_id, mate), device_id_type=MESH).wait_recv()
        return carry
    lax.fori_loop(1, n_dev, e_wait, 0)
    e_ref[0] = jnp.sum(ebuf[...])

    def e_sent(step, carry):
        e_copy(step).wait_send()
        return carry
    lax.fori_loop(1, n_dev, e_sent, 0)

    def sent(idx, carry):
        remote(0, send_sem.at[idx], recv_sem.at[0, 0], mate).wait_send()
        return carry
    lax.fori_loop(0, len(sends), sent, 0)

    def mate_sent(idx, carry):
        remote(0, dsend_sem.at[lax.div(idx, TILES), lax.rem(idx, TILES)], drecv_sem.at[0, 0], mate).wait_send()
        return carry
    lax.fori_loop(0, TILES * (len(STAGES) + 1), mate_sent, 0)


def solution(mesh):
    n_dev = mesh.shape['row']
    assert n_dev == 2 * SIDE * SIDE

    def per_device(positions, charges, counts):
        rows, width = positions.shape
        assert rows == TILE * TILES and 2 * width == TILE
        n_sends = sum(len(relay_list(k)) for k in range(-1, len(STAGES)))
        hbm = pl.BlockSpec(memory_space=pltpu.HBM)
        smem = pl.BlockSpec(memory_space=pltpu.SMEM)
        force, energy = pl.pallas_call(
            functools.partial(kernel, width),
            out_shape=[jax.ShapeDtypeStruct((rows, width), F32), jax.ShapeDtypeStruct((1,), F32)],
            in_specs=[hbm, hbm, smem],
            out_specs=[pl.BlockSpec(memory_space=pltpu.VMEM), smem],
            scratch_shapes=[
                pltpu.VMEM((rows, width), BF16),
                pltpu.VMEM((rows // width, width), F32),
                pltpu.SemaphoreType.DMA((2,)),
                pltpu.VMEM((n_dev * TILES, width + AUG, TILE), BF16),
                pltpu.VMEM((rows, 2 * width), BF16),
                pltpu.VMEM((rows, width), F32),
                pltpu.VMEM((rows, width), F32),
                pltpu.VMEM((rows, width), F32),
                pltpu.VMEM((n_dev, 8, width), F32),
                pltpu.SemaphoreType.DMA((n_sends,)),
                pltpu.SemaphoreType.DMA((len(STAGES), TILES)),
                pltpu.SemaphoreType.DMA((len(STAGES) + 1, TILES)),
                pltpu.SemaphoreType.DMA((len(STAGES) + 1, TILES)),
                pltpu.SemaphoreType.DMA((n_dev,)),
                pltpu.SemaphoreType.DMA((n_dev,)),
            ],
            compiler_params=pltpu.CompilerParams(collective_id=0, has_side_effects=True),
            name='pair_forces',
        )(positions, charges.reshape(rows // width, width), counts)
        return force, energy

    row_spec = P(('sys', 'row'), None)
    vec_spec = P(('sys', 'row'))
    return jax.shard_map(per_device, mesh=mesh, in_specs=(row_spec, vec_spec, vec_spec),
                         out_specs=(row_spec, P('sys')), check_vma=False)
```

```python
import functools
import math

import jax
import jax.numpy as jnp
from jax import lax
from jax.experimental import pallas as pl
from jax.experimental.pallas import tpu as pltpu
from jax.sharding import PartitionSpec as P

MESH = pl.DeviceIdType.MESH
BF16, F32 = jnp.bfloat16, jnp.float32
TILE = 256
AUG = 16
S_CAP = 1.69e38
C_CAP = 3.3895313892515355e38

SIDE, TILES = 4, 4
PAIRS = [(0, 2), (1, 1), (1, -1), (-1, 1), (-1, -1), (2, 0), (1, 2), (-1, 2), (2, 1), (2, -1), (2, 2)]
STAGES = [[((0, 1), t), ((0, -1), t), ((1, 0), t + 2), ((-1, 0), t + 2)] for t in (0, 1)]
STAGES += [[((1, 0), t), ((-1, 0), t), ((0, 1), t + 2), ((0, -1), t + 2)] for t in (0, 1)]
STAGES += [[((a, b), 0), ((a, b), 1), ((b, a), 2), ((b, a), 3)] for a, b in PAIRS]
STAGE_OF = {piece: k for k, stage in enumerate(STAGES) for piece in stage}
SHARE = (0.5, 0.5, 0.5, 0.5, 0.5, 1.0, 0.5, 0.5, 0.0, 0.5, 1.0, 0.0, 1.0, 0.0, 0.5)
COMPUTE = (0, 1, 2, 3, 4, 5, 6, 7, 10, 9, 12, 14, 8, 11, 13)
ARRIVALS = {0: (1,), 1: (2,), 2: (3,), 3: (4,), 4: (5, 6), 5: (7, 8), 6: (10, 11), 7: (9,), 8: (12,), 9: (14, 13)}
ENERGY_AT = 12


def wrap(d):
    return (d + 1) % SIDE - 1


def relays(piece):
    (slow, fast), t = piece
    swap = t >= TILES // 2
    if swap:
        slow, fast = fast, slow
    lead = 1 if t % 2 == 0 else -1
    hops = []
    if slow == 0 and fast == 0:
        hops += [(0, 1), (0, -1)]
    elif slow == 0 and fast == lead:
        hops += [(0, -fast)]
    if slow == 0:
        hops += [(1, 0), (-1, 0)]
    elif slow == lead:
        hops += [(-slow, 0)]
    return [(b, a) if swap else (a, b) for a, b in hops]


def relay_list(k):
    pieces = [((0, 0), t) for t in range(TILES)] if k < 0 else STAGES[k]
    found = []
    for piece in pieces:
        swap = piece[1] >= TILES // 2
        for hop in relays(piece):
            along = hop[1] if not swap else hop[0]
            found.append((0 if along else 1, len(found), piece, hop))
    return [(piece, hop) for _, _, piece, hop in sorted(found)]


def merged(copies, join):
    found = []
    for piece, hop in copies:
        left = (piece[0], piece[1] - 1)
        if join and piece[1] % 2 == 1 and (left, 1, hop) in found:
            found[found.index((left, 1, hop))] = (left, 2, hop)
        else:
            found.append((piece, 1, hop))
    return found


def dot(lhs, rhs, dims):
    return lax.dot_general(lhs, rhs, (dims, ((), ())), preferred_element_type=F32)


def split3(val):
    hi = jnp.clip(val, -C_CAP, C_CAP).astype(BF16).astype(F32)
    mid = (val - hi).astype(BF16).astype(F32)
    low = (val - hi - mid).astype(BF16).astype(F32)
    return hi, mid, low


def kernel(width, x_hbm, q_hbm, cnt_ref, out_ref, e_ref, x_ref, q_ref, in_sem, slots, xa, ci, s_acc, t_acc, ebuf,
           send_sem, recv_sem, mate_sem, e_sem):
    rows = x_ref.shape[0]
    n_dev = 2 * SIDE * SIDE
    n_steps = len(STAGES)
    n_sends = sum(len(relay_list(k)) for k in range(-1, len(STAGES)))
    me = lax.axis_index('row')
    sys_id = lax.axis_index('sys')
    core = lax.rem(me, 2)
    chip = lax.div(me, 2)
    pos_y, pos_x = lax.div(chip, SIDE), lax.rem(chip, SIDE)
    mate = me + 1 - 2 * core
    scale = math.log2(math.e) / width

    def dev(dy, dx, plane):
        return (lax.rem(pos_y + dy + SIDE, SIDE) * SIDE + lax.rem(pos_x + dx + SIDE, SIDE)) * 2 + plane

    x_in = pltpu.make_async_copy(x_hbm, x_ref, in_sem.at[0])
    q_in = pltpu.make_async_copy(q_hbm, q_ref, in_sem.at[1])
    x_in.start()
    q_in.start()
    barrier = pltpu.get_barrier_semaphore()
    near = [dev(0, 1, core), dev(0, -1, core), dev(1, 0, core), dev(-1, 0, core), mate]
    for peer in near:
        pl.semaphore_signal(barrier, inc=1, device_id=(sys_id, peer), device_id_type=MESH)
    s_acc[...] = jnp.zeros_like(s_acc)
    t_acc[...] = jnp.zeros_like(t_acc)
    x_in.wait()
    q_in.wait()

    count = cnt_ref[0]
    row_id = lax.broadcasted_iota(jnp.int32, (rows, width), 0)
    lane_id = lax.broadcasted_iota(jnp.int32, (rows, width), 1)
    x_val = jnp.where(row_id < count, x_ref[...].astype(F32), 0.0)
    x_t = x_val.T
    s_row = -jnp.minimum(0.5 * jnp.sum(x_t * x_t, axis=0, keepdims=True), S_CAP)
    q_shape = q_ref.shape
    q_id = lax.broadcasted_iota(jnp.int32, q_shape, 0) * q_shape[1] + lax.broadcasted_iota(jnp.int32, q_shape, 1)
    q_val = jnp.where(q_id < count, q_ref[...], 0.0)
    q_row = jnp.concatenate([q_val[r:r + 1, :] for r in range(q_shape[0])], axis=1)
    aug_id = lax.broadcasted_iota(jnp.int32, (AUG, rows), 0)
    aug = jnp.where(aug_id < 3, 1.0, 0.0)
    for k, part in enumerate(split3(s_row) + split3(q_row)):
        aug = jnp.where(aug_id == 3 + k, part, aug)
    for t in range(TILES):
        cols = slice(t * TILE, (t + 1) * TILE)
        slots[me * TILES + t, :width, :] = x_t[:, cols].astype(BF16)
        slots[me * TILES + t, width:, :] = aug[:, cols].astype(BF16)
    pl.semaphore_wait(barrier, len(near))

    def unit_of(piece, plane):
        return dev(piece[0][0], piece[0][1], plane) * TILES + piece[1]

    def remote(unit, tiles, send, recv, peer):
        ref = slots.at[pl.ds(unit, tiles)]
        return pltpu.make_async_remote_copy(src_ref=ref, dst_ref=ref, send_sem=send, recv_sem=recv,
                                            device_id=(sys_id, peer), device_id_type=MESH)

    def start_relays(k):
        for piece, tiles, hop in merged(relay_list(k), k >= 0):
            there = ((wrap(piece[0][0] - hop[0]), wrap(piece[0][1] - hop[1])), piece[1])
            remote(unit_of(piece, core), tiles, send_sem.at[0], recv_sem.at[STAGE_OF[there]],
                   dev(hop[0], hop[1], core)).start()

    def to_mate(k):
        if k < 0:
            groups = [(((0, 0), 0), TILES, None)]
        else:
            groups = merged([(piece, None) for piece in STAGES[k]], True)
        for piece, tiles, _ in groups:
            remote(unit_of(piece, core), tiles, send_sem.at[1], mate_sem.at[k + 1], mate).start()

    def arrive(k):
        remote(0, TILES, send_sem.at[0], recv_sem.at[k], mate).wait_recv()
        start_relays(k)
        to_mate(k)

    def from_mate(k):
        remote(0, TILES, send_sem.at[1], mate_sem.at[k + 1], mate).wait_recv()

    start_relays(-1)
    to_mate(-1)

    s_col = -jnp.minimum(0.5 * jnp.sum(x_val * x_val, axis=1, keepdims=True), S_CAP)
    xa[:, :width] = x_val.astype(BF16)
    tail = jnp.where((lane_id >= 3) & (lane_id < 6), 1.0, 0.0)
    for k, part in enumerate(split3(s_col)):
        tail = jnp.where(lane_id == k, part, tail)
    xa[:, width:] = tail.astype(BF16)
    q_t = q_val.T
    for r in range(q_shape[0]):
        lanes = q_shape[1]
        ci[r * lanes:(r + 1) * lanes, :] = jnp.broadcast_to(q_t[:, r:r + 1], (lanes, width))

    eye = (lax.broadcasted_iota(jnp.int32, (TILE, TILE), 0) == lax.broadcasted_iota(jnp.int32, (TILE, TILE), 1))
    pad = jnp.zeros((width - AUG, TILE), BF16)

    def column_tile(unit, diag=None):
        block = slots[unit]
        rhs = jnp.concatenate([block, pad], axis=0)
        parts = block[width:, :].astype(F32)
        c_cols = parts[6:7, :] + parts[7:8, :] + parts[8:9, :]
        for it in range(rows // TILE):
            mine = slice(it * TILE, (it + 1) * TILE)
            arg = dot(xa[mine, :], rhs, ((1,), (0,)))
            weight = jnp.exp2(jnp.minimum(arg, 0.0) * scale) * c_cols
            if it == diag:
                weight = jnp.where(eye, 0.0, weight)
            c_mine = ci[mine, :]
            left, right = weight[:, :width] * c_mine, weight[:, width:] * c_mine
            s_acc[mine, :] += left + right
            w_low = jnp.concatenate([left, right], axis=1).astype(BF16)
            t_acc[mine, :] += dot(w_low, block[:width, :], ((1,), (1,)))

    for t in range(TILES):
        column_tile(me * TILES + t, diag=t)
    arrive(0)
    from_mate(-1)
    for t in range(TILES):
        column_tile(mate * TILES + t)
    ebuf[me] = jnp.zeros(ebuf.shape[1:], F32)

    def e_copy(first, count, peer):
        ref = ebuf.at[pl.ds(first, count)]
        return pltpu.make_async_remote_copy(src_ref=ref, dst_ref=ref, send_sem=e_sem.at[0], recv_sem=e_sem.at[1],
                                            device_id=(sys_id, peer), device_id_type=MESH)

    def e_start(step, carry):
        e_copy(me, 1, lax.rem(me + step, n_dev)).start()
        return carry

    def tally(weight):
        ebuf[me] += weight * jnp.sum(s_acc[...].reshape(rows // 8, 8, width), axis=0)

    share = [0.5] + [SHARE[k] for k in COMPUTE]

    def step_units(step):
        units = []
        for j in range(TILES):
            code = jnp.int32(0)
            for now, k in enumerate(COMPUTE):
                (dy, dx), t = STAGES[k][j]
                code = jnp.where(step == now, ((dy % SIDE) * SIDE + dx % SIDE) * TILES + t, code)
            for plane in (core, 1 - core):
                units.append(dev(lax.div(code, SIDE * TILES), lax.rem(lax.div(code, TILES), SIDE), plane) * TILES
                             + lax.rem(code, TILES))
        return units

    def step_body(step, carry):
        for now in range(n_steps):
            @pl.when(step == now)
            def _():
                for k in ARRIVALS.get(now, ()):
                    arrive(k)
                from_mate(COMPUTE[now])
                if now <= ENERGY_AT and share[now] != share[now + 1]:
                    tally(share[now] - share[now + 1])
                if now == ENERGY_AT:
                    lax.fori_loop(1, n_dev, e_start, 0)
        for unit in step_units(step):
            column_tile(unit)
        return carry
    lax.fori_loop(0, n_steps, step_body, 0)

    s_sum = jnp.sum(s_acc[...], axis=1, keepdims=True)
    out_ref[...] = (s_sum * xa[:, :width].astype(F32) - t_acc[...]) * (1.0 / width)

    e_copy(0, n_dev - 1, mate).wait_recv()
    e_ref[0] = jnp.sum(ebuf[...])
    e_copy(0, n_dev - 1, mate).wait_send()
    remote(0, n_sends, send_sem.at[0], recv_sem.at[0], mate).wait_send()
    remote(0, TILES * (len(STAGES) + 1), send_sem.at[1], mate_sem.at[0], mate).wait_send()


def solution(mesh):
    n_dev = mesh.shape['row']
    assert n_dev == 2 * SIDE * SIDE

    def per_device(positions, charges, counts):
        rows, width = positions.shape
        assert rows == TILE * TILES and 2 * width == TILE
        hbm = pl.BlockSpec(memory_space=pltpu.HBM)
        smem = pl.BlockSpec(memory_space=pltpu.SMEM)
        force, energy = pl.pallas_call(
            functools.partial(kernel, width),
            out_shape=[jax.ShapeDtypeStruct((rows, width), F32), jax.ShapeDtypeStruct((1,), F32)],
            in_specs=[hbm, hbm, smem],
            out_specs=[pl.BlockSpec(memory_space=pltpu.VMEM), smem],
            scratch_shapes=[
                pltpu.VMEM((rows, width), BF16),
                pltpu.VMEM((rows // width, width), F32),
                pltpu.SemaphoreType.DMA((2,)),
                pltpu.VMEM((n_dev * TILES, width + AUG, TILE), BF16),
                pltpu.VMEM((rows, 2 * width), BF16),
                pltpu.VMEM((rows, width), F32),
                pltpu.VMEM((rows, width), F32),
                pltpu.VMEM((rows, width), F32),
                pltpu.VMEM((n_dev, 8, width), F32),
                pltpu.SemaphoreType.DMA((2,)),
                pltpu.SemaphoreType.DMA((len(STAGES),)),
                pltpu.SemaphoreType.DMA((len(STAGES) + 1,)),
                pltpu.SemaphoreType.DMA((2,)),
            ],
            compiler_params=pltpu.CompilerParams(collective_id=0, has_side_effects=True),
            name='pair_forces',
        )(positions, charges.reshape(rows // width, width), counts)
        return force, energy

    row_spec = P(('sys', 'row'), None)
    vec_spec = P(('sys', 'row'))
    return jax.shard_map(per_device, mesh=mesh, in_specs=(row_spec, vec_spec, vec_spec),
                         out_specs=(row_spec, P('sys')), check_vma=False)
```

```python
import functools
import math

import jax
import jax.numpy as jnp
from jax import lax
from jax.experimental import pallas as pl
from jax.experimental.pallas import tpu as pltpu
from jax.sharding import PartitionSpec as P

MESH = pl.DeviceIdType.MESH
BF16, F32 = jnp.bfloat16, jnp.float32
TILE = 256
AUG = 16
S_CAP = 1.69e38
C_CAP = 3.3895313892515355e38

SIDE, TILES = 4, 4
PAIRS = [(0, 2), (1, 1), (1, -1), (-1, 1), (-1, -1), (2, 0), (1, 2), (-1, 2), (2, 1), (2, -1), (2, 2)]
STAGES = [[((0, 1), t), ((0, -1), t), ((1, 0), t + 2), ((-1, 0), t + 2)] for t in (0, 1)]
STAGES += [[((1, 0), t), ((-1, 0), t), ((0, 1), t + 2), ((0, -1), t + 2)] for t in (0, 1)]
STAGES += [[((a, b), 0), ((a, b), 1), ((b, a), 2), ((b, a), 3)] for a, b in PAIRS]
STAGE_OF = {piece: k for k, stage in enumerate(STAGES) for piece in stage}
SHARE = (0.5, 0.5, 0.5, 0.5, 0.5, 1.0, 0.5, 0.5, 0.0, 0.5, 1.0, 0.0, 1.0, 0.0, 0.5)
LOOPS = [
    [((1,), (0,)), ((2,), (1,)), ((3,), (2,)), ((4,), (3,)), ((5, 6), (4,)), ((7, 8), (5,)), ((), (8,))],
    [((10, 11, 9, 12), (6, 7)), ((14, 13), (10, 12)), ((), (9, 14)), ((), (11, 13))],
]


def wrap(d):
    return (d + 1) % SIDE - 1


def relays(piece):
    (slow, fast), t = piece
    swap = t >= TILES // 2
    if swap:
        slow, fast = fast, slow
    lead = 1 if t % 2 == 0 else -1
    hops = []
    if slow == 0 and fast == 0:
        hops += [(0, 1), (0, -1)]
    elif slow == 0 and fast == lead:
        hops += [(0, -fast)]
    if slow == 0:
        hops += [(1, 0), (-1, 0)]
    elif slow == lead:
        hops += [(-slow, 0)]
    return [(b, a) if swap else (a, b) for a, b in hops]


def relay_list(k):
    pieces = [((0, 0), t) for t in range(TILES)] if k < 0 else STAGES[k]
    found = []
    for piece in pieces:
        swap = piece[1] >= TILES // 2
        for hop in relays(piece):
            along = hop[1] if not swap else hop[0]
            found.append((0 if along else 1, len(found), piece, hop))
    return [(piece, hop) for _, _, piece, hop in sorted(found)]


def merged(copies, join):
    found = []
    for piece, hop in copies:
        left = (piece[0], piece[1] - 1)
        if join and piece[1] % 2 == 1 and (left, 1, hop) in found:
            found[found.index((left, 1, hop))] = (left, 2, hop)
        else:
            found.append((piece, 1, hop))
    return found


def dot(lhs, rhs, dims):
    return lax.dot_general(lhs, rhs, (dims, ((), ())), preferred_element_type=F32)


def split3(val):
    hi = jnp.clip(val, -C_CAP, C_CAP).astype(BF16).astype(F32)
    mid = (val - hi).astype(BF16).astype(F32)
    low = (val - hi - mid).astype(BF16).astype(F32)
    return hi, mid, low


def kernel(width, x_hbm, q_hbm, cnt_ref, out_ref, e_ref, x_ref, q_ref, in_sem, slots, xa, ci, s_acc, t_acc, ebuf,
           send_sem, recv_sem, mate_sem, e_sem):
    rows = x_ref.shape[0]
    n_dev = 2 * SIDE * SIDE
    n_sends = sum(len(relay_list(k)) for k in range(-1, len(STAGES)))
    me = lax.axis_index('row')
    sys_id = lax.axis_index('sys')
    core = lax.rem(me, 2)
    chip = lax.div(me, 2)
    pos_y, pos_x = lax.div(chip, SIDE), lax.rem(chip, SIDE)
    mate = me + 1 - 2 * core
    scale = math.log2(math.e) / width

    def dev(dy, dx, plane):
        return (lax.rem(pos_y + dy + SIDE, SIDE) * SIDE + lax.rem(pos_x + dx + SIDE, SIDE)) * 2 + plane

    x_in = pltpu.make_async_copy(x_hbm, x_ref, in_sem.at[0])
    q_in = pltpu.make_async_copy(q_hbm, q_ref, in_sem.at[1])
    x_in.start()
    q_in.start()
    barrier = pltpu.get_barrier_semaphore()
    near = [dev(0, 1, core), dev(0, -1, core), dev(1, 0, core), dev(-1, 0, core), mate]
    for peer in near:
        pl.semaphore_signal(barrier, inc=1, device_id=(sys_id, peer), device_id_type=MESH)
    s_acc[...] = jnp.zeros_like(s_acc)
    t_acc[...] = jnp.zeros_like(t_acc)
    x_in.wait()
    q_in.wait()

    count = cnt_ref[0]
    row_id = lax.broadcasted_iota(jnp.int32, (rows, width), 0)
    lane_id = lax.broadcasted_iota(jnp.int32, (rows, width), 1)
    x_val = jnp.where(row_id < count, x_ref[...].astype(F32), 0.0)
    x_t = x_val.T
    s_row = -jnp.minimum(0.5 * jnp.sum(x_t * x_t, axis=0, keepdims=True), S_CAP)
    q_shape = q_ref.shape
    q_id = lax.broadcasted_iota(jnp.int32, q_shape, 0) * q_shape[1] + lax.broadcasted_iota(jnp.int32, q_shape, 1)
    q_val = jnp.where(q_id < count, q_ref[...], 0.0)
    q_row = jnp.concatenate([q_val[r:r + 1, :] for r in range(q_shape[0])], axis=1)
    aug_id = lax.broadcasted_iota(jnp.int32, (AUG, rows), 0)
    aug = jnp.where(aug_id < 3, 1.0, 0.0)
    for k, part in enumerate(split3(s_row) + split3(q_row)):
        aug = jnp.where(aug_id == 3 + k, part, aug)
    for t in range(TILES):
        cols = slice(t * TILE, (t + 1) * TILE)
        slots[me * TILES + t, :width, :] = x_t[:, cols].astype(BF16)
        slots[me * TILES + t, width:, :] = aug[:, cols].astype(BF16)
    pl.semaphore_wait(barrier, len(near))

    def unit_of(piece, plane):
        return dev(piece[0][0], piece[0][1], plane) * TILES + piece[1]

    def remote(unit, tiles, send, recv, peer):
        ref = slots.at[pl.ds(unit, tiles)]
        return pltpu.make_async_remote_copy(src_ref=ref, dst_ref=ref, send_sem=send, recv_sem=recv,
                                            device_id=(sys_id, peer), device_id_type=MESH)

    def start_relays(k):
        for piece, tiles, hop in merged(relay_list(k), k >= 0):
            there = ((wrap(piece[0][0] - hop[0]), wrap(piece[0][1] - hop[1])), piece[1])
            remote(unit_of(piece, core), tiles, send_sem.at[0], recv_sem.at[STAGE_OF[there]],
                   dev(hop[0], hop[1], core)).start()

    def to_mate(k):
        if k < 0:
            groups = [(((0, 0), 0), TILES, None)]
        else:
            groups = merged([(piece, None) for piece in STAGES[k]], True)
        for piece, tiles, _ in groups:
            remote(unit_of(piece, core), tiles, send_sem.at[1], mate_sem.at[k + 1], mate).start()

    def arrive(k):
        remote(0, TILES, send_sem.at[0], recv_sem.at[k], mate).wait_recv()
        start_relays(k)
        to_mate(k)

    def from_mate(k):
        remote(0, TILES, send_sem.at[1], mate_sem.at[k + 1], mate).wait_recv()

    start_relays(-1)
    to_mate(-1)

    s_col = -jnp.minimum(0.5 * jnp.sum(x_val * x_val, axis=1, keepdims=True), S_CAP)
    xa[:, :width] = x_val.astype(BF16)
    tail = jnp.where((lane_id >= 3) & (lane_id < 6), 1.0, 0.0)
    for k, part in enumerate(split3(s_col)):
        tail = jnp.where(lane_id == k, part, tail)
    xa[:, width:] = tail.astype(BF16)
    q_t = q_val.T
    for r in range(q_shape[0]):
        lanes = q_shape[1]
        ci[r * lanes:(r + 1) * lanes, :] = jnp.broadcast_to(q_t[:, r:r + 1], (lanes, width))

    eye = (lax.broadcasted_iota(jnp.int32, (TILE, TILE), 0) == lax.broadcasted_iota(jnp.int32, (TILE, TILE), 1))
    pad = jnp.zeros((width - AUG, TILE), BF16)

    def column_tile(unit, diag=None):
        block = slots[unit]
        rhs = jnp.concatenate([block, pad], axis=0)
        parts = block[width:, :].astype(F32)
        c_cols = parts[6:7, :] + parts[7:8, :] + parts[8:9, :]
        for it in range(rows // TILE):
            mine = slice(it * TILE, (it + 1) * TILE)
            arg = dot(xa[mine, :], rhs, ((1,), (0,)))
            weight = jnp.exp2(jnp.minimum(arg, 0.0) * scale) * c_cols
            if it == diag:
                weight = jnp.where(eye, 0.0, weight)
            c_mine = ci[mine, :]
            left, right = weight[:, :width] * c_mine, weight[:, width:] * c_mine
            s_acc[mine, :] += left + right
            w_low = jnp.concatenate([left, right], axis=1).astype(BF16)
            t_acc[mine, :] += dot(w_low, block[:width, :], ((1,), (1,)))

    for t in range(TILES):
        column_tile(me * TILES + t, diag=t)
    arrive(0)
    from_mate(-1)
    for t in range(TILES):
        column_tile(mate * TILES + t)
    ebuf[me] = jnp.zeros(ebuf.shape[1:], F32)

    def e_copy(first, count, peer):
        ref = ebuf.at[pl.ds(first, count)]
        return pltpu.make_async_remote_copy(src_ref=ref, dst_ref=ref, send_sem=e_sem.at[0], recv_sem=e_sem.at[1],
                                            device_id=(sys_id, peer), device_id_type=MESH)

    def e_start(step, carry):
        e_copy(me, 1, lax.rem(me + step, n_dev)).start()
        return carry

    def tally(weight):
        ebuf[me] += weight * jnp.sum(s_acc[...].reshape(rows // 8, 8, width), axis=0)

    def step_units(steps, step, i):
        units = []
        for j in range(TILES):
            code = jnp.int32(0)
            for now, (_, computed) in enumerate(steps):
                (dy, dx), t = STAGES[computed[i]][j]
                code = jnp.where(step == now, ((dy % SIDE) * SIDE + dx % SIDE) * TILES + t, code)
            for plane in (core, 1 - core):
                units.append(dev(lax.div(code, SIDE * TILES), lax.rem(lax.div(code, TILES), SIDE), plane) * TILES
                             + lax.rem(code, TILES))
        return units

    def run_loop(steps, share, share_after):
        shares = [share] + [SHARE[computed[0]] for _, computed in steps]

        def step_body(step, carry):
            for now, (arriving, computed) in enumerate(steps):
                @pl.when(step == now)
                def _():
                    for k in arriving:
                        arrive(k)
                    for k in computed:
                        assert SHARE[k] == SHARE[computed[0]]
                        from_mate(k)
                    if shares[now] != shares[now + 1]:
                        tally(shares[now] - shares[now + 1])
                    if share_after is None and now == len(steps) - 1:
                        assert SHARE[computed[0]] == 0.0
                        lax.fori_loop(1, n_dev, e_start, 0)
            for i in range(len(steps[0][1])):
                for unit in step_units(steps, step, i):
                    column_tile(unit)
            return carry
        lax.fori_loop(0, len(steps), step_body, 0)
        return shares[-1]

    last_share = 0.5
    for n, steps in enumerate(LOOPS):
        last_share = run_loop(steps, last_share, None if n == len(LOOPS) - 1 else 1)

    s_sum = jnp.sum(s_acc[...], axis=1, keepdims=True)
    out_ref[...] = (s_sum * xa[:, :width].astype(F32) - t_acc[...]) * (1.0 / width)

    e_copy(0, n_dev - 1, mate).wait_recv()
    e_ref[0] = jnp.sum(ebuf[...])
    e_copy(0, n_dev - 1, mate).wait_send()
    remote(0, n_sends, send_sem.at[0], recv_sem.at[0], mate).wait_send()
    remote(0, TILES * (len(STAGES) + 1), send_sem.at[1], mate_sem.at[0], mate).wait_send()


def solution(mesh):
    n_dev = mesh.shape['row']
    assert n_dev == 2 * SIDE * SIDE

    def per_device(positions, charges, counts):
        rows, width = positions.shape
        assert rows == TILE * TILES and 2 * width == TILE
        hbm = pl.BlockSpec(memory_space=pltpu.HBM)
        smem = pl.BlockSpec(memory_space=pltpu.SMEM)
        force, energy = pl.pallas_call(
            functools.partial(kernel, width),
            out_shape=[jax.ShapeDtypeStruct((rows, width), F32), jax.ShapeDtypeStruct((1,), F32)],
            in_specs=[hbm, hbm, smem],
            out_specs=[pl.BlockSpec(memory_space=pltpu.VMEM), smem],
            scratch_shapes=[
                pltpu.VMEM((rows, width), BF16),
                pltpu.VMEM((rows // width, width), F32),
                pltpu.SemaphoreType.DMA((2,)),
                pltpu.VMEM((n_dev * TILES, width + AUG, TILE), BF16),
                pltpu.VMEM((rows, 2 * width), BF16),
                pltpu.VMEM((rows, width), F32),
                pltpu.VMEM((rows, width), F32),
                pltpu.VMEM((rows, width), F32),
                pltpu.VMEM((n_dev, 8, width), F32),
                pltpu.SemaphoreType.DMA((2,)),
                pltpu.SemaphoreType.DMA((len(STAGES),)),
                pltpu.SemaphoreType.DMA((len(STAGES) + 1,)),
                pltpu.SemaphoreType.DMA((2,)),
            ],
            compiler_params=pltpu.CompilerParams(collective_id=0, has_side_effects=True),
            name='pair_forces',
        )(positions, charges.reshape(rows // width, width), counts)
        return force, energy

    row_spec = P(('sys', 'row'), None)
    vec_spec = P(('sys', 'row'))
    return jax.shard_map(per_device, mesh=mesh, in_specs=(row_spec, vec_spec, vec_spec),
                         out_specs=(row_spec, P('sys')), check_vma=False)
```

```python
import functools
import math

import jax
import jax.numpy as jnp
from jax import lax
from jax.experimental import pallas as pl
from jax.experimental.pallas import tpu as pltpu
from jax.sharding import PartitionSpec as P

MESH = pl.DeviceIdType.MESH
BF16, F32 = jnp.bfloat16, jnp.float32
TILE = 256
AUG = 16
S_CAP = 1.69e38
C_CAP = 3.3895313892515355e38

SIDE, TILES = 4, 4
PAIRS = [(2, 0), (1, 2), (-1, 2), (2, 1), (2, -1), (2, 2)]
STAGES = [[((0, 1), t), ((0, -1), t), ((1, 0), t + 2), ((-1, 0), t + 2)] for t in (0, 1)]
STAGES += [[((1, 0), t), ((-1, 0), t), ((0, 1), t + 2), ((0, -1), t + 2)] for t in (0, 1)]
CORNERS = [[((1, s), t), ((-1, s), t), ((s, 1), t + 2), ((s, -1), t + 2)] for t in (0, 1) for s in (1, -1)]
STAGES += CORNERS[:2] + [[((0, 2), 0), ((0, 2), 1), ((2, 0), 2), ((2, 0), 3)]] + CORNERS[2:]
STAGES += [[((a, b), 0), ((a, b), 1), ((b, a), 2), ((b, a), 3)] for a, b in PAIRS]
STAGE_OF = {piece: k for k, stage in enumerate(STAGES) for piece in stage}
SHARE = (0.5, 0.5, 0.5, 0.5, 0.5, 0.5, 0.5, 0.5, 0.5, 0.5, 1.0, 0.0, 1.0, 0.0, 0.5)
RELAYS = {0: ((0, (0,)),), 1: ((1, (0,)), (0, (1,)), (1, (1,)))}
LOOPS = [
    [((1,), (0,)), ((2,), (1,)), ((3,), (2,)), ((6, 4), (3,)), ((5,), (6,))],
    [((7, 8), (4, 5)), ((9, 10, 11), (7, 8)), ((12, 13, 14), (9, 10)), ((), (12, 14)), ((), (11, 13))],
]


def wrap(d):
    return (d + 1) % SIDE - 1


def relays(piece):
    (slow, fast), t = piece
    swap = t >= TILES // 2
    if swap:
        slow, fast = fast, slow
    lead = 1 if t % 2 == 0 else -1
    hops = []
    if slow == 0 and fast == 0:
        hops += [(0, 1), (0, -1)]
    elif slow == 0 and fast == lead:
        hops += [(0, -fast)]
    if slow == 0:
        hops += [(1, 0), (-1, 0)]
    elif slow == lead:
        hops += [(-slow, 0)]
    return [(b, a) if swap else (a, b) for a, b in hops]


def relay_list(k, ranks=(0, 1)):
    pieces = [((0, 0), t) for t in range(TILES)] if k < 0 else STAGES[k]
    found = []
    for piece in pieces:
        swap = piece[1] >= TILES // 2
        for hop in relays(piece):
            along = hop[1] if not swap else hop[0]
            found.append((0 if along else 1, len(found), piece, hop))
    return [(piece, hop) for rank, _, piece, hop in sorted(found) if rank in ranks]


def merged(copies, join):
    found = []
    for piece, hop in copies:
        left = (piece[0], piece[1] - 1)
        if join and piece[1] % 2 == 1 and (left, 1, hop) in found:
            found[found.index((left, 1, hop))] = (left, 2, hop)
        else:
            found.append((piece, 1, hop))
    return found


def dot(lhs, rhs, dims):
    return lax.dot_general(lhs, rhs, (dims, ((), ())), preferred_element_type=F32)


def split3(val):
    hi = jnp.clip(val, -C_CAP, C_CAP).astype(BF16).astype(F32)
    mid = (val - hi).astype(BF16).astype(F32)
    low = (val - hi - mid).astype(BF16).astype(F32)
    return hi, mid, low


def kernel(width, x_hbm, q_hbm, cnt_ref, out_ref, e_ref, x_ref, q_ref, in_sem, slots, xa, ci, s_acc, t_acc, e_acc, ebuf,
           send_sem, recv_sem, mate_sem, e_sem):
    rows = x_ref.shape[0]
    n_dev = 2 * SIDE * SIDE
    n_sends = sum(len(relay_list(k)) for k in range(-1, len(STAGES)))
    me = lax.axis_index('row')
    sys_id = lax.axis_index('sys')
    core = lax.rem(me, 2)
    chip = lax.div(me, 2)
    pos_y, pos_x = lax.div(chip, SIDE), lax.rem(chip, SIDE)
    mate = me + 1 - 2 * core
    scale = math.log2(math.e) / width

    def dev(dy, dx, plane):
        return (lax.rem(pos_y + dy + SIDE, SIDE) * SIDE + lax.rem(pos_x + dx + SIDE, SIDE)) * 2 + plane

    x_in = pltpu.make_async_copy(x_hbm, x_ref, in_sem.at[0])
    q_in = pltpu.make_async_copy(q_hbm, q_ref, in_sem.at[1])
    x_in.start()
    q_in.start()
    barrier = pltpu.get_barrier_semaphore()
    near = [dev(0, 1, core), dev(0, -1, core), dev(1, 0, core), dev(-1, 0, core), mate]
    for peer in near:
        pl.semaphore_signal(barrier, inc=1, device_id=(sys_id, peer), device_id_type=MESH)
    s_acc[...] = jnp.zeros_like(s_acc)
    t_acc[...] = jnp.zeros_like(t_acc)
    x_in.wait()
    q_in.wait()

    count = cnt_ref[0]
    row_id = lax.broadcasted_iota(jnp.int32, (rows, width), 0)
    lane_id = lax.broadcasted_iota(jnp.int32, (rows, width), 1)
    x_val = jnp.where(row_id < count, x_ref[...].astype(F32), 0.0)
    x_t = x_val.T
    s_row = -jnp.minimum(0.5 * jnp.sum(x_t * x_t, axis=0, keepdims=True), S_CAP)
    q_shape = q_ref.shape
    q_id = lax.broadcasted_iota(jnp.int32, q_shape, 0) * q_shape[1] + lax.broadcasted_iota(jnp.int32, q_shape, 1)
    q_val = jnp.where(q_id < count, q_ref[...], 0.0)
    q_row = jnp.concatenate([q_val[r:r + 1, :] for r in range(q_shape[0])], axis=1)
    aug_id = lax.broadcasted_iota(jnp.int32, (AUG, rows), 0)
    aug = jnp.where(aug_id < 3, 1.0, 0.0)
    for k, part in enumerate(split3(s_row) + split3(q_row)):
        aug = jnp.where(aug_id == 3 + k, part, aug)
    for t in range(TILES):
        cols = slice(t * TILE, (t + 1) * TILE)
        slots[me * TILES + t, :width, :] = x_t[:, cols].astype(BF16)
        slots[me * TILES + t, width:, :] = aug[:, cols].astype(BF16)
    pl.semaphore_wait(barrier, len(near))

    def unit_of(piece, plane):
        return dev(piece[0][0], piece[0][1], plane) * TILES + piece[1]

    def remote(unit, tiles, send, recv, peer):
        ref = slots.at[pl.ds(unit, tiles)]
        return pltpu.make_async_remote_copy(src_ref=ref, dst_ref=ref, send_sem=send, recv_sem=recv,
                                            device_id=(sys_id, peer), device_id_type=MESH)

    def start_relays(k, ranks):
        for piece, tiles, hop in merged(relay_list(k, ranks), k >= 0):
            there = ((wrap(piece[0][0] - hop[0]), wrap(piece[0][1] - hop[1])), piece[1])
            remote(unit_of(piece, core), tiles, send_sem.at[0], recv_sem.at[STAGE_OF[there]],
                   dev(hop[0], hop[1], core)).start()

    def to_mate(k):
        if k < 0:
            groups = [(((0, 0), 0), TILES, None)]
        else:
            groups = merged([(piece, None) for piece in STAGES[k]], True)
        for piece, tiles, _ in groups:
            remote(unit_of(piece, core), tiles, send_sem.at[1], mate_sem.at[k + 1], mate).start()

    def arrive(k):
        remote(0, TILES, send_sem.at[0], recv_sem.at[k], mate).wait_recv()
        for other, ranks in RELAYS.get(k, ((k, (0, 1)),)):
            start_relays(other, ranks)
        to_mate(k)

    def from_mate(k):
        remote(0, TILES, send_sem.at[1], mate_sem.at[k + 1], mate).wait_recv()

    start_relays(-1, (0, 1))
    to_mate(-1)

    s_col = -jnp.minimum(0.5 * jnp.sum(x_val * x_val, axis=1, keepdims=True), S_CAP)
    xa[:, :width] = x_val.astype(BF16)
    tail = jnp.where((lane_id >= 3) & (lane_id < 6), 1.0, 0.0)
    for k, part in enumerate(split3(s_col)):
        tail = jnp.where(lane_id == k, part, tail)
    xa[:, width:] = tail.astype(BF16)
    q_t = q_val.T
    for r in range(q_shape[0]):
        lanes = q_shape[1]
        ci[r * lanes:(r + 1) * lanes, :] = jnp.broadcast_to(q_t[:, r:r + 1], (lanes, width))

    eye = (lax.broadcasted_iota(jnp.int32, (TILE, TILE), 0) == lax.broadcasted_iota(jnp.int32, (TILE, TILE), 1))
    pad = jnp.zeros((width - AUG, TILE), BF16)

    def column_tile(unit, diag=None):
        block = slots[unit]
        rhs = jnp.concatenate([block, pad], axis=0)
        parts = block[width:, :].astype(F32)
        c_cols = parts[6:7, :] + parts[7:8, :] + parts[8:9, :]
        for it in range(rows // TILE):
            mine = slice(it * TILE, (it + 1) * TILE)
            arg = dot(xa[mine, :], rhs, ((1,), (0,)))
            weight = jnp.exp2(jnp.minimum(arg, 0.0) * scale) * c_cols
            if it == diag:
                weight = jnp.where(eye, 0.0, weight)
            c_mine = ci[mine, :]
            left, right = weight[:, :width] * c_mine, weight[:, width:] * c_mine
            s_acc[mine, :] += left + right
            w_low = jnp.concatenate([left, right], axis=1).astype(BF16)
            t_acc[mine, :] += dot(w_low, block[:width, :], ((1,), (1,)))

    for t in range(TILES):
        column_tile(me * TILES + t, diag=t)
    arrive(0)
    from_mate(-1)
    for t in range(TILES):
        column_tile(mate * TILES + t)
    e_acc[...] = jnp.zeros_like(e_acc)

    def e_copy(first, count, peer):
        ref = ebuf.at[pl.ds(first, count)]
        return pltpu.make_async_remote_copy(src_ref=ref, dst_ref=ref, send_sem=e_sem.at[0], recv_sem=e_sem.at[1],
                                            device_id=(sys_id, peer), device_id_type=MESH)

    def e_start(step, carry):
        e_copy(me, 1, lax.rem(me + step, n_dev)).start()
        return carry

    def tally(weight):
        e_acc[...] += weight * jnp.sum(s_acc[...].reshape(rows // 8, 8, width), axis=0)

    def step_units(steps, step, i):
        units = []
        for j in range(TILES):
            code = jnp.int32(0)
            for now, (_, computed) in enumerate(steps):
                (dy, dx), t = STAGES[computed[i]][j]
                code = jnp.where(step == now, ((dy % SIDE) * SIDE + dx % SIDE) * TILES + t, code)
            for plane in (core, 1 - core):
                units.append(dev(lax.div(code, SIDE * TILES), lax.rem(lax.div(code, TILES), SIDE), plane) * TILES
                             + lax.rem(code, TILES))
        return units

    def run_loop(steps, share, share_after):
        shares = [share] + [SHARE[computed[-1]] for _, computed in steps]
        starts = [SHARE[computed[0]] for _, computed in steps]
        inner = [SHARE[computed[0]] - SHARE[computed[-1]] for _, computed in steps]

        def step_body(step, carry):
            for now, (arriving, computed) in enumerate(steps):
                @pl.when(step == now)
                def _():
                    for k in arriving:
                        arrive(k)
                    for k in computed:
                        from_mate(k)
                    if shares[now] != starts[now]:
                        tally(shares[now] - starts[now])
                    if share_after is None and now == len(steps) - 1:
                        assert not any(SHARE[k] for k in computed)
                        ebuf[me] = e_acc[...]
                        lax.fori_loop(1, n_dev, e_start, 0)
            for i in range(len(steps[0][1])):
                if i and any(inner):
                    weight = jnp.float32(0.0)
                    for now, change in enumerate(inner):
                        weight = jnp.where(step == now, change, weight)
                    tally(weight)
                for unit in step_units(steps, step, i):
                    column_tile(unit)
            return carry
        lax.fori_loop(0, len(steps), step_body, 0)
        return shares[-1]

    last_share = 0.5
    for n, steps in enumerate(LOOPS):
        last_share = run_loop(steps, last_share, None if n == len(LOOPS) - 1 else 1)

    s_sum = jnp.sum(s_acc[...], axis=1, keepdims=True)
    out_ref[...] = (s_sum * xa[:, :width].astype(F32) - t_acc[...]) * (1.0 / width)

    e_copy(0, n_dev - 1, mate).wait_recv()
    e_ref[0] = jnp.sum(ebuf[...])
    e_copy(0, n_dev - 1, mate).wait_send()
    remote(0, n_sends, send_sem.at[0], recv_sem.at[0], mate).wait_send()
    remote(0, TILES * (len(STAGES) + 1), send_sem.at[1], mate_sem.at[0], mate).wait_send()


def solution(mesh):
    n_dev = mesh.shape['row']
    assert n_dev == 2 * SIDE * SIDE

    def per_device(positions, charges, counts):
        rows, width = positions.shape
        assert rows == TILE * TILES and 2 * width == TILE
        hbm = pl.BlockSpec(memory_space=pltpu.HBM)
        smem = pl.BlockSpec(memory_space=pltpu.SMEM)
        force, energy = pl.pallas_call(
            functools.partial(kernel, width),
            out_shape=[jax.ShapeDtypeStruct((rows, width), F32), jax.ShapeDtypeStruct((1,), F32)],
            in_specs=[hbm, hbm, smem],
            out_specs=[pl.BlockSpec(memory_space=pltpu.VMEM), smem],
            scratch_shapes=[
                pltpu.VMEM((rows, width), BF16),
                pltpu.VMEM((rows // width, width), F32),
                pltpu.SemaphoreType.DMA((2,)),
                pltpu.VMEM((n_dev * TILES, width + AUG, TILE), BF16),
                pltpu.VMEM((rows, 2 * width), BF16),
                pltpu.VMEM((rows, width), F32),
                pltpu.VMEM((rows, width), F32),
                pltpu.VMEM((rows, width), F32),
                pltpu.VMEM((8, width), F32),
                pltpu.VMEM((n_dev, 8, width), F32),
                pltpu.SemaphoreType.DMA((2,)),
                pltpu.SemaphoreType.DMA((len(STAGES),)),
                pltpu.SemaphoreType.DMA((len(STAGES) + 1,)),
                pltpu.SemaphoreType.DMA((2,)),
            ],
            compiler_params=pltpu.CompilerParams(collective_id=0, has_side_effects=True),
            name='pair_forces',
        )(positions, charges.reshape(rows // width, width), counts)
        return force, energy

    row_spec = P(('sys', 'row'), None)
    vec_spec = P(('sys', 'row'))
    return jax.shard_map(per_device, mesh=mesh, in_specs=(row_spec, vec_spec, vec_spec),
                         out_specs=(row_spec, P('sys')), check_vma=False)
```

```python
import functools
import math

import jax
import jax.numpy as jnp
from jax import lax
from jax.experimental import pallas as pl
from jax.experimental.pallas import tpu as pltpu
from jax.sharding import PartitionSpec as P

MESH = pl.DeviceIdType.MESH
BF16, F32 = jnp.bfloat16, jnp.float32
TILE = 256
AUG = 16
S_CAP = 1.69e38
C_CAP = 3.3895313892515355e38

SIDE, TILES = 4, 4
PAIRS = [(2, 0), (1, 2), (-1, 2), (2, 1), (2, -1), (2, 2)]
STAGES = [[((0, 1), t), ((0, -1), t), ((1, 0), t + 2), ((-1, 0), t + 2)] for t in (0, 1)]
STAGES += [[((1, 0), t), ((-1, 0), t), ((0, 1), t + 2), ((0, -1), t + 2)] for t in (0, 1)]
CORNERS = [[((1, s), t), ((-1, s), t), ((s, 1), t + 2), ((s, -1), t + 2)] for t in (0, 1) for s in (1, -1)]
STAGES += CORNERS[:2] + [[((0, 2), 0), ((0, 2), 1), ((2, 0), 2), ((2, 0), 3)]] + CORNERS[2:]
STAGES += [[((a, b), 0), ((a, b), 1), ((b, a), 2), ((b, a), 3)] for a, b in PAIRS]
STAGE_OF = {piece: (k, j) for k, stage in enumerate(STAGES) for j, piece in enumerate(stage)}
STAGE_OF.update({((0, 0), t): (-1, t) for t in range(TILES)})
SHARE = (0.5, 0.5, 0.5, 0.5, 0.5, 0.5, 0.5, 0.5, 0.5, 0.5, 1.0, 0.0, 1.0, 0.0, 0.5)
RELAYS = {0: ((0, (0,)),), 1: ((1, (0,)), (0, (1,)), (1, (1,)))}
LOOPS = [
    [((1,), (0,)), ((2,), (1,)), ((3,), (2,)), ((6, 4), (3,)), ((5,), (6,))],
    [((7, 8), (4, 5)), ((9, 10, 11), (7, 8)), ((12, 13, 14), (9, 10)), ((), (12, 14)), ((), (11, 13))],
]


PLACE = {k: n for n, k in enumerate([-1] + [k for steps in LOOPS for _, computed in steps for k in computed])}


def wrap(d):
    return (d + 1) % SIDE - 1


def relays(piece):
    (slow, fast), t = piece
    swap = t >= TILES // 2
    if swap:
        slow, fast = fast, slow
    lead = 1 if t % 2 == 0 else -1
    hops = []
    if slow == 0 and fast == 0:
        hops += [(0, 1), (0, -1)]
    elif slow == 0 and fast == lead:
        hops += [(0, -fast)]
    if slow == 0:
        hops += [(1, 0), (-1, 0)]
    elif slow == lead:
        hops += [(-slow, 0)]
    return [(b, a) if swap else (a, b) for a, b in hops]


def relay_list(k, ranks=(0, 1)):
    pieces = [((0, 0), t) for t in range(TILES)] if k < 0 else STAGES[k]
    found = []
    for piece in pieces:
        swap = piece[1] >= TILES // 2
        for hop in relays(piece):
            along = hop[1] if not swap else hop[0]
            found.append((0 if along else 1, len(found), piece, hop))
    return [(piece, hop) for rank, _, piece, hop in sorted(found) if rank in ranks]


def merged(copies, join):
    found = []
    for piece, hop in copies:
        left = (piece[0], piece[1] - 1)
        beside = join and piece[1] % 2 == 1 and STAGE_OF[left][0] == STAGE_OF[piece][0]
        if beside and (left, 1, hop) in found:
            found[found.index((left, 1, hop))] = (left, 2, hop)
        else:
            found.append((piece, 1, hop))
    return found


def dot(lhs, rhs, dims):
    return lax.dot_general(lhs, rhs, (dims, ((), ())), preferred_element_type=F32)


def split3(val):
    hi = jnp.clip(val, -C_CAP, C_CAP).astype(BF16).astype(F32)
    mid = (val - hi).astype(BF16).astype(F32)
    low = (val - hi - mid).astype(BF16).astype(F32)
    return hi, mid, low


def kernel(width, x_hbm, q_hbm, cnt_ref, out_ref, e_ref, x_ref, q_ref, in_sem, slots, xa, ci, s_acc, t_acc, e_acc, ebuf,
           send_sem, recv_sem, mate_sem, e_sem):
    rows = x_ref.shape[0]
    n_dev = 2 * SIDE * SIDE
    n_sends = sum(len(relay_list(k)) for k in range(-1, len(STAGES)))
    me = lax.axis_index('row')
    sys_id = lax.axis_index('sys')
    core = lax.rem(me, 2)
    chip = lax.div(me, 2)
    pos_y, pos_x = lax.div(chip, SIDE), lax.rem(chip, SIDE)
    mate = me + 1 - 2 * core
    scale = math.log2(math.e) / width

    def dev(dy, dx, plane):
        return (lax.rem(pos_y + dy + SIDE, SIDE) * SIDE + lax.rem(pos_x + dx + SIDE, SIDE)) * 2 + plane

    x_in = pltpu.make_async_copy(x_hbm, x_ref, in_sem.at[0])
    q_in = pltpu.make_async_copy(q_hbm, q_ref, in_sem.at[1])
    x_in.start()
    q_in.start()
    barrier = pltpu.get_barrier_semaphore()
    near = [dev(0, 1, core), dev(0, -1, core), dev(1, 0, core), dev(-1, 0, core), mate]
    for peer in near:
        pl.semaphore_signal(barrier, inc=1, device_id=(sys_id, peer), device_id_type=MESH)
    s_acc[...] = jnp.zeros_like(s_acc)
    t_acc[...] = jnp.zeros_like(t_acc)
    x_in.wait()
    q_in.wait()

    count = cnt_ref[0]
    row_id = lax.broadcasted_iota(jnp.int32, (rows, width), 0)
    lane_id = lax.broadcasted_iota(jnp.int32, (rows, width), 1)
    x_val = jnp.where(row_id < count, x_ref[...].astype(F32), 0.0)
    x_t = x_val.T
    s_row = -jnp.minimum(0.5 * jnp.sum(x_t * x_t, axis=0, keepdims=True), S_CAP)
    q_shape = q_ref.shape
    q_id = lax.broadcasted_iota(jnp.int32, q_shape, 0) * q_shape[1] + lax.broadcasted_iota(jnp.int32, q_shape, 1)
    q_val = jnp.where(q_id < count, q_ref[...], 0.0)
    q_row = jnp.concatenate([q_val[r:r + 1, :] for r in range(q_shape[0])], axis=1)
    aug_id = lax.broadcasted_iota(jnp.int32, (AUG, rows), 0)
    aug = jnp.where(aug_id < 3, 1.0, 0.0)
    for k, part in enumerate(split3(s_row) + split3(q_row)):
        aug = jnp.where(aug_id == 3 + k, part, aug)
    for t in range(TILES):
        cols = slice(t * TILE, (t + 1) * TILE)
        slots[t, :width, :] = x_t[:, cols].astype(BF16)
        slots[t, width:, :] = aug[:, cols].astype(BF16)
    pl.semaphore_wait(barrier, len(near))

    other = n_dev // 2 * TILES

    def unit_of(piece):
        k, j = STAGE_OF[piece]
        return PLACE[k] * TILES + j

    def remote(src, dst, tiles, send, recv, peer):
        return pltpu.make_async_remote_copy(
            src_ref=slots.at[pl.ds(src, tiles)], dst_ref=slots.at[pl.ds(dst, tiles)], send_sem=send, recv_sem=recv,
            device_id=(sys_id, peer), device_id_type=MESH)

    def start_relays(k, ranks):
        for piece, tiles, hop in merged(relay_list(k, ranks), k >= 0):
            there = ((wrap(piece[0][0] - hop[0]), wrap(piece[0][1] - hop[1])), piece[1])
            remote(unit_of(piece), unit_of(there), tiles, send_sem.at[0], recv_sem.at[STAGE_OF[there][0]],
                   dev(hop[0], hop[1], core)).start()

    def to_mate(k):
        first = PLACE[k] * TILES
        remote(first, other + first, TILES, send_sem.at[1], mate_sem.at[k + 1], mate).start()

    def arrive(k):
        remote(0, PLACE[k] * TILES, TILES, send_sem.at[0], recv_sem.at[k], mate).wait_recv()
        for stage, ranks in RELAYS.get(k, ((k, (0, 1)),)):
            start_relays(stage, ranks)
        to_mate(k)

    def from_mate(k):
        remote(0, other + PLACE[k] * TILES, TILES, send_sem.at[1], mate_sem.at[k + 1], mate).wait_recv()

    start_relays(-1, (0, 1))
    to_mate(-1)

    s_col = -jnp.minimum(0.5 * jnp.sum(x_val * x_val, axis=1, keepdims=True), S_CAP)
    xa[:, :width] = x_val.astype(BF16)
    tail = jnp.where((lane_id >= 3) & (lane_id < 6), 1.0, 0.0)
    for k, part in enumerate(split3(s_col)):
        tail = jnp.where(lane_id == k, part, tail)
    xa[:, width:] = tail.astype(BF16)
    q_t = q_val.T
    for r in range(q_shape[0]):
        lanes = q_shape[1]
        ci[r * lanes:(r + 1) * lanes, :] = jnp.broadcast_to(q_t[:, r:r + 1], (lanes, width))

    eye = (lax.broadcasted_iota(jnp.int32, (TILE, TILE), 0) == lax.broadcasted_iota(jnp.int32, (TILE, TILE), 1))
    pad = jnp.zeros((width - AUG, TILE), BF16)

    def column_tile(unit, diag=None):
        block = slots[unit]
        rhs = jnp.concatenate([block, pad], axis=0)
        parts = block[width:, :].astype(F32)
        c_cols = parts[6:7, :] + parts[7:8, :] + parts[8:9, :]
        for it in range(rows // TILE):
            mine = slice(it * TILE, (it + 1) * TILE)
            arg = dot(xa[mine, :], rhs, ((1,), (0,)))
            weight = jnp.exp2(jnp.minimum(arg, 0.0) * scale) * c_cols
            if it == diag:
                weight = jnp.where(eye, 0.0, weight)
            c_mine = ci[mine, :]
            left, right = weight[:, :width] * c_mine, weight[:, width:] * c_mine
            s_acc[mine, :] += left + right
            w_low = jnp.concatenate([left, right], axis=1).astype(BF16)
            t_acc[mine, :] += dot(w_low, block[:width, :], ((1,), (1,)))

    for t in range(TILES):
        column_tile(t, diag=t)
    arrive(0)
    from_mate(-1)
    for t in range(TILES):
        column_tile(other + t)
    e_acc[...] = jnp.zeros_like(e_acc)

    def e_copy(first, count, peer):
        ref = ebuf.at[pl.ds(first, count)]
        return pltpu.make_async_remote_copy(src_ref=ref, dst_ref=ref, send_sem=e_sem.at[0], recv_sem=e_sem.at[1],
                                            device_id=(sys_id, peer), device_id_type=MESH)

    def e_start(step, carry):
        e_copy(me, 1, lax.rem(me + step, n_dev)).start()
        return carry

    def tally(weight):
        e_acc[...] += weight * jnp.sum(s_acc[...].reshape(rows // 8, 8, width), axis=0)

    def run_loop(steps, share, share_after):
        shares = [share] + [SHARE[computed[-1]] for _, computed in steps]
        starts = [SHARE[computed[0]] for _, computed in steps]
        inner = [SHARE[computed[0]] - SHARE[computed[-1]] for _, computed in steps]

        def step_body(step, carry):
            for now, (arriving, computed) in enumerate(steps):
                @pl.when(step == now)
                def _():
                    for k in arriving:
                        arrive(k)
                    for k in computed:
                        from_mate(k)
                    if shares[now] != starts[now]:
                        tally(shares[now] - starts[now])
                    if share_after is None and now == len(steps) - 1:
                        assert not any(SHARE[k] for k in computed)
                        ebuf[me] = e_acc[...]
                        lax.fori_loop(1, n_dev, e_start, 0)
            for i in range(len(steps[0][1])):
                if i and any(inner):
                    weight = jnp.float32(0.0)
                    for now, change in enumerate(inner):
                        weight = jnp.where(step == now, change, weight)
                    tally(weight)
                first = (PLACE[steps[0][1][0]] + step * len(steps[0][1]) + i) * TILES
                for j in range(TILES):
                    column_tile(first + j)
                    column_tile(other + first + j)
            return carry
        lax.fori_loop(0, len(steps), step_body, 0)
        return shares[-1]

    last_share = 0.5
    for n, steps in enumerate(LOOPS):
        last_share = run_loop(steps, last_share, None if n == len(LOOPS) - 1 else 1)

    s_sum = jnp.sum(s_acc[...], axis=1, keepdims=True)
    out_ref[...] = (s_sum * xa[:, :width].astype(F32) - t_acc[...]) * (1.0 / width)

    e_copy(0, n_dev - 1, mate).wait_recv()
    e_ref[0] = jnp.sum(ebuf[...])
    e_copy(0, n_dev - 1, mate).wait_send()
    remote(0, 0, n_sends, send_sem.at[0], recv_sem.at[0], mate).wait_send()
    remote(0, 0, other, send_sem.at[1], mate_sem.at[0], mate).wait_send()


def solution(mesh):
    n_dev = mesh.shape['row']
    assert n_dev == 2 * SIDE * SIDE

    def per_device(positions, charges, counts):
        rows, width = positions.shape
        assert rows == TILE * TILES and 2 * width == TILE
        hbm = pl.BlockSpec(memory_space=pltpu.HBM)
        smem = pl.BlockSpec(memory_space=pltpu.SMEM)
        force, energy = pl.pallas_call(
            functools.partial(kernel, width),
            out_shape=[jax.ShapeDtypeStruct((rows, width), F32), jax.ShapeDtypeStruct((1,), F32)],
            in_specs=[hbm, hbm, smem],
            out_specs=[pl.BlockSpec(memory_space=pltpu.VMEM), smem],
            scratch_shapes=[
                pltpu.VMEM((rows, width), BF16),
                pltpu.VMEM((rows // width, width), F32),
                pltpu.SemaphoreType.DMA((2,)),
                pltpu.VMEM((n_dev * TILES, width + AUG, TILE), BF16),
                pltpu.VMEM((rows, 2 * width), BF16),
                pltpu.VMEM((rows, width), F32),
                pltpu.VMEM((rows, width), F32),
                pltpu.VMEM((rows, width), F32),
                pltpu.VMEM((8, width), F32),
                pltpu.VMEM((n_dev, 8, width), F32),
                pltpu.SemaphoreType.DMA((2,)),
                pltpu.SemaphoreType.DMA((len(STAGES),)),
                pltpu.SemaphoreType.DMA((len(STAGES) + 1,)),
                pltpu.SemaphoreType.DMA((2,)),
            ],
            compiler_params=pltpu.CompilerParams(collective_id=0, has_side_effects=True),
            name='pair_forces',
        )(positions, charges.reshape(rows // width, width), counts)
        return force, energy

    row_spec = P(('sys', 'row'), None)
    vec_spec = P(('sys', 'row'))
    return jax.shard_map(per_device, mesh=mesh, in_specs=(row_spec, vec_spec, vec_spec),
                         out_specs=(row_spec, P('sys')), check_vma=False)
```

```python
import functools
import math

import jax
import jax.numpy as jnp
from jax import lax
from jax.experimental import pallas as pl
from jax.experimental.pallas import tpu as pltpu
from jax.sharding import PartitionSpec as P

MESH = pl.DeviceIdType.MESH
BF16, F32 = jnp.bfloat16, jnp.float32
TILE = 256
AUG = 16
S_CAP = 1.69e38
C_CAP = 3.3895313892515355e38

SIDE, TILES = 4, 4
PAIRS = [(2, 0), (1, 2), (-1, 2), (2, 1), (2, -1), (2, 2)]
STAGES = [[((0, 1), t), ((0, -1), t), ((1, 0), t + 2), ((-1, 0), t + 2)] for t in (0, 1)]
STAGES += [[((1, 0), t), ((-1, 0), t), ((0, 1), t + 2), ((0, -1), t + 2)] for t in (0, 1)]
CORNERS = [[((1, s), t), ((-1, s), t), ((s, 1), t + 2), ((s, -1), t + 2)] for t in (0, 1) for s in (1, -1)]
STAGES += CORNERS[:2] + [[((0, 2), 0), ((0, 2), 1), ((2, 0), 2), ((2, 0), 3)]] + CORNERS[2:]
STAGES += [[((a, b), 0), ((a, b), 1), ((b, a), 2), ((b, a), 3)] for a, b in PAIRS]
STAGE_OF = {piece: (k, j) for k, stage in enumerate(STAGES) for j, piece in enumerate(stage)}
STAGE_OF.update({((0, 0), t): (-1, t) for t in range(TILES)})
SHARE = (0.5, 0.5, 0.5, 0.5, 0.5, 0.5, 0.5, 0.5, 0.5, 0.5, 1.0, 0.0, 1.0, 0.0, 0.5)
RELAYS = {0: ((0, (0,)),), 1: ((1, (0,)), (0, (1,)), (1, (1,)))}
LOOPS = [
    [((1,), (0,)), ((2,), (1,)), ((3,), (2,)), ((6, 4), (3,)), ((5,), (6,))],
    [((7, 8), (4, 5)), ((9, 10, 11), (7, 8)), ((12, 13, 14), (9, 10)), ((), (12, 14)), ((), (11, 13))],
]


PLACE = {k: n for n, k in enumerate([-1] + [k for steps in LOOPS for _, computed in steps for k in computed])}


def wrap(d):
    return (d + 1) % SIDE - 1


def relays(piece):
    (slow, fast), t = piece
    swap = t >= TILES // 2
    if swap:
        slow, fast = fast, slow
    lead = 1 if t % 2 == 0 else -1
    hops = []
    if slow == 0 and fast == 0:
        hops += [(0, 1), (0, -1)]
    elif slow == 0 and fast == lead:
        hops += [(0, -fast)]
    if slow == 0:
        hops += [(1, 0), (-1, 0)]
    elif slow == lead:
        hops += [(-slow, 0)]
    return [(b, a) if swap else (a, b) for a, b in hops]


def relay_list(k, ranks=(0, 1)):
    pieces = [((0, 0), t) for t in range(TILES)] if k < 0 else STAGES[k]
    found = []
    for piece in pieces:
        swap = piece[1] >= TILES // 2
        for hop in relays(piece):
            along = hop[1] if not swap else hop[0]
            found.append((0 if along else 1, len(found), piece, hop))
    return [(piece, hop) for rank, _, piece, hop in sorted(found) if rank in ranks]


def merged(copies, join):
    found = []
    for piece, hop in copies:
        left = (piece[0], piece[1] - 1)
        beside = join and piece[1] % 2 == 1 and STAGE_OF[left][0] == STAGE_OF[piece][0]
        if beside and (left, 1, hop) in found:
            found[found.index((left, 1, hop))] = (left, 2, hop)
        else:
            found.append((piece, 1, hop))
    return found


def dot(lhs, rhs, dims):
    return lax.dot_general(lhs, rhs, (dims, ((), ())), preferred_element_type=F32)


def split3(val):
    hi = jnp.clip(val, -C_CAP, C_CAP).astype(BF16).astype(F32)
    mid = (val - hi).astype(BF16).astype(F32)
    low = (val - hi - mid).astype(BF16).astype(F32)
    return hi, mid, low


def kernel(width, x_hbm, q_hbm, cnt_ref, out_ref, e_ref, x_ref, q_ref, in_sem, slots, xa, ci, s_acc, t_acc, e_acc, ebuf,
           send_sem, recv_sem, mate_sem, e_sem):
    rows = x_ref.shape[0]
    n_dev = 2 * SIDE * SIDE
    n_sends = sum(len(relay_list(k)) for k in range(-1, len(STAGES)))
    me = lax.axis_index('row')
    sys_id = lax.axis_index('sys')
    core = lax.rem(me, 2)
    chip = lax.div(me, 2)
    pos_y, pos_x = lax.div(chip, SIDE), lax.rem(chip, SIDE)
    mate = me + 1 - 2 * core
    scale = math.log2(math.e) / width

    def dev(dy, dx, plane):
        return (lax.rem(pos_y + dy + SIDE, SIDE) * SIDE + lax.rem(pos_x + dx + SIDE, SIDE)) * 2 + plane

    x_in = pltpu.make_async_copy(x_hbm, x_ref, in_sem.at[0])
    q_in = pltpu.make_async_copy(q_hbm, q_ref, in_sem.at[1])
    x_in.start()
    q_in.start()
    barrier = pltpu.get_barrier_semaphore()
    near = [dev(0, 1, core), dev(0, -1, core), dev(1, 0, core), dev(-1, 0, core), mate]
    for peer in near:
        pl.semaphore_signal(barrier, inc=1, device_id=(sys_id, peer), device_id_type=MESH)
    s_acc[...] = jnp.zeros_like(s_acc)
    t_acc[...] = jnp.zeros_like(t_acc)
    x_in.wait()
    q_in.wait()

    count = cnt_ref[0]
    row_id = lax.broadcasted_iota(jnp.int32, (rows, width), 0)
    lane_id = lax.broadcasted_iota(jnp.int32, (rows, width), 1)
    x_val = jnp.where(row_id < count, x_ref[...].astype(F32), 0.0)
    x_t = x_val.T
    s_row = -jnp.minimum(0.5 * jnp.sum(x_t * x_t, axis=0, keepdims=True), S_CAP)
    q_shape = q_ref.shape
    q_id = lax.broadcasted_iota(jnp.int32, q_shape, 0) * q_shape[1] + lax.broadcasted_iota(jnp.int32, q_shape, 1)
    q_val = jnp.where(q_id < count, q_ref[...], 0.0)
    q_row = jnp.concatenate([q_val[r:r + 1, :] for r in range(q_shape[0])], axis=1)
    aug_id = lax.broadcasted_iota(jnp.int32, (AUG, rows), 0)
    aug = jnp.where(aug_id < 3, 1.0, 0.0)
    for k, part in enumerate(split3(s_row) + split3(q_row)):
        aug = jnp.where(aug_id == 3 + k, part, aug)
    for t in range(TILES):
        cols = slice(t * TILE, (t + 1) * TILE)
        slots[t, :width, :] = x_t[:, cols].astype(BF16)
        slots[t, width:, :] = aug[:, cols].astype(BF16)
    pl.semaphore_wait(barrier, len(near))

    other = n_dev // 2 * TILES

    def unit_of(piece):
        k, j = STAGE_OF[piece]
        return PLACE[k] * TILES + j

    def remote(src, dst, tiles, send, recv, peer):
        return pltpu.make_async_remote_copy(
            src_ref=slots.at[pl.ds(src, tiles)], dst_ref=slots.at[pl.ds(dst, tiles)], send_sem=send, recv_sem=recv,
            device_id=(sys_id, peer), device_id_type=MESH)

    def start_relays(k, ranks):
        for piece, tiles, hop in merged(relay_list(k, ranks), k >= 0):
            there = ((wrap(piece[0][0] - hop[0]), wrap(piece[0][1] - hop[1])), piece[1])
            remote(unit_of(piece), unit_of(there), tiles, send_sem.at[0], recv_sem.at[STAGE_OF[there][0]],
                   dev(hop[0], hop[1], core)).start()

    def to_mate(k):
        first = PLACE[k] * TILES
        remote(first, other + first, TILES, send_sem.at[1], mate_sem.at[k + 1], mate).start()

    def arrive(k):
        remote(0, PLACE[k] * TILES, TILES, send_sem.at[0], recv_sem.at[k], mate).wait_recv()
        for stage, ranks in RELAYS.get(k, ((k, (0, 1)),)):
            start_relays(stage, ranks)
        to_mate(k)

    def from_mate(k):
        remote(0, other + PLACE[k] * TILES, TILES, send_sem.at[1], mate_sem.at[k + 1], mate).wait_recv()

    start_relays(-1, (0, 1))
    to_mate(-1)

    s_col = -jnp.minimum(0.5 * jnp.sum(x_val * x_val, axis=1, keepdims=True), S_CAP)
    xa[:, :width] = x_val.astype(BF16)
    tail = jnp.where((lane_id >= 3) & (lane_id < 6), 1.0, 0.0)
    for k, part in enumerate(split3(s_col)):
        tail = jnp.where(lane_id == k, part, tail)
    xa[:, width:] = tail.astype(BF16)
    q_t = q_val.T
    for r in range(q_shape[0]):
        lanes = q_shape[1]
        ci[r * lanes:(r + 1) * lanes, :] = jnp.broadcast_to(q_t[:, r:r + 1], (lanes, width))

    eye = (lax.broadcasted_iota(jnp.int32, (TILE, TILE), 0) == lax.broadcasted_iota(jnp.int32, (TILE, TILE), 1))
    pad = jnp.zeros((width - AUG, TILE), BF16)

    def column_tile(unit, diag=None):
        block = slots[unit]
        rhs = jnp.concatenate([block, pad], axis=0)
        parts = block[width:, :].astype(F32)
        c_cols = parts[6:7, :] + parts[7:8, :] + parts[8:9, :]
        for it in range(rows // TILE):
            mine = slice(it * TILE, (it + 1) * TILE)
            arg = dot(xa[mine, :], rhs, ((1,), (0,)))
            weight = jnp.exp2(jnp.minimum(arg, 0.0) * scale) * c_cols
            if it == diag:
                weight = jnp.where(eye, 0.0, weight)
            c_mine = ci[mine, :]
            left, right = weight[:, :width] * c_mine, weight[:, width:] * c_mine
            s_acc[mine, :] += left + right
            w_low = jnp.concatenate([left, right], axis=1).astype(BF16)
            t_acc[mine, :] += dot(w_low, block[:width, :], ((1,), (1,)))

    for t in range(TILES):
        column_tile(t, diag=t)
    from_mate(-1)
    for t in range(TILES):
        column_tile(other + t)
    e_acc[...] = jnp.zeros_like(e_acc)
    arrive(0)
    for t in range(TILES):
        column_tile(TILES + t)

    early = LOOPS[0]
    assert all(SHARE[k] == 0.5 for _, computed in early for k in computed)

    def early_body(step, carry):
        for now, (arriving, computed) in enumerate(early[:-1]):
            @pl.when(step == now)
            def _():
                for k in arriving:
                    arrive(k)
                from_mate(computed[0])
        for j in range(TILES):
            column_tile(other + (step + 1) * TILES + j)
            column_tile((step + 2) * TILES + j)
        return carry
    lax.fori_loop(0, len(early) - 1, early_body, 0)
    for k in early[-1][0]:
        arrive(k)
    from_mate(early[-1][1][0])
    for j in range(TILES):
        column_tile(other + len(early) * TILES + j)

    def e_copy(first, count, peer):
        ref = ebuf.at[pl.ds(first, count)]
        return pltpu.make_async_remote_copy(src_ref=ref, dst_ref=ref, send_sem=e_sem.at[0], recv_sem=e_sem.at[1],
                                            device_id=(sys_id, peer), device_id_type=MESH)

    def e_start(step, carry):
        e_copy(me, 1, lax.rem(me + step, n_dev)).start()
        return carry

    def tally(weight):
        e_acc[...] += weight * jnp.sum(s_acc[...].reshape(rows // 8, 8, width), axis=0)

    def run_loop(steps, share, share_after):
        shares = [share] + [SHARE[computed[-1]] for _, computed in steps]
        starts = [SHARE[computed[0]] for _, computed in steps]
        inner = [SHARE[computed[0]] - SHARE[computed[-1]] for _, computed in steps]

        def step_body(step, carry):
            for now, (arriving, computed) in enumerate(steps):
                @pl.when(step == now)
                def _():
                    for k in arriving:
                        arrive(k)
                    for k in computed:
                        from_mate(k)
                    if shares[now] != starts[now]:
                        tally(shares[now] - starts[now])
                    if share_after is None and now == len(steps) - 1:
                        assert not any(SHARE[k] for k in computed)
                        ebuf[me] = e_acc[...]
                        lax.fori_loop(1, n_dev, e_start, 0)
            for i in range(len(steps[0][1])):
                if i and any(inner):
                    weight = jnp.float32(0.0)
                    for now, change in enumerate(inner):
                        weight = jnp.where(step == now, change, weight)
                    tally(weight)
                first = (PLACE[steps[0][1][0]] + step * len(steps[0][1]) + i) * TILES
                for j in range(TILES):
                    column_tile(first + j)
                    column_tile(other + first + j)
            return carry
        lax.fori_loop(0, len(steps), step_body, 0)
        return shares[-1]

    run_loop(LOOPS[1], 0.5, None)

    s_sum = jnp.sum(s_acc[...], axis=1, keepdims=True)
    out_ref[...] = (s_sum * xa[:, :width].astype(F32) - t_acc[...]) * (1.0 / width)

    e_copy(0, n_dev - 1, mate).wait_recv()
    e_ref[0] = jnp.sum(ebuf[...])
    e_copy(0, n_dev - 1, mate).wait_send()
    remote(0, 0, n_sends, send_sem.at[0], recv_sem.at[0], mate).wait_send()
    remote(0, 0, other, send_sem.at[1], mate_sem.at[0], mate).wait_send()


def solution(mesh):
    n_dev = mesh.shape['row']
    assert n_dev == 2 * SIDE * SIDE

    def per_device(positions, charges, counts):
        rows, width = positions.shape
        assert rows == TILE * TILES and 2 * width == TILE
        hbm = pl.BlockSpec(memory_space=pltpu.HBM)
        smem = pl.BlockSpec(memory_space=pltpu.SMEM)
        force, energy = pl.pallas_call(
            functools.partial(kernel, width),
            out_shape=[jax.ShapeDtypeStruct((rows, width), F32), jax.ShapeDtypeStruct((1,), F32)],
            in_specs=[hbm, hbm, smem],
            out_specs=[pl.BlockSpec(memory_space=pltpu.VMEM), smem],
            scratch_shapes=[
                pltpu.VMEM((rows, width), BF16),
                pltpu.VMEM((rows // width, width), F32),
                pltpu.SemaphoreType.DMA((2,)),
                pltpu.VMEM((n_dev * TILES, width + AUG, TILE), BF16),
                pltpu.VMEM((rows, 2 * width), BF16),
                pltpu.VMEM((rows, width), F32),
                pltpu.VMEM((rows, width), F32),
                pltpu.VMEM((rows, width), F32),
                pltpu.VMEM((8, width), F32),
                pltpu.VMEM((n_dev, 8, width), F32),
                pltpu.SemaphoreType.DMA((2,)),
                pltpu.SemaphoreType.DMA((len(STAGES),)),
                pltpu.SemaphoreType.DMA((len(STAGES) + 1,)),
                pltpu.SemaphoreType.DMA((2,)),
            ],
            compiler_params=pltpu.CompilerParams(collective_id=0, has_side_effects=True),
            name='pair_forces',
        )(positions, charges.reshape(rows // width, width), counts)
        return force, energy

    row_spec = P(('sys', 'row'), None)
    vec_spec = P(('sys', 'row'))
    return jax.shard_map(per_device, mesh=mesh, in_specs=(row_spec, vec_spec, vec_spec),
                         out_specs=(row_spec, P('sys')), check_vma=False)
```

```python
import functools
import math

import jax
import jax.numpy as jnp
from jax import lax
from jax.experimental import pallas as pl
from jax.experimental.pallas import tpu as pltpu
from jax.sharding import PartitionSpec as P

MESH = pl.DeviceIdType.MESH
BF16, F32 = jnp.bfloat16, jnp.float32
TILE = 256
AUG = 16
S_CAP = 1.69e38
C_CAP = 3.3895313892515355e38

SIDE, TILES = 4, 4
PAIRS = [(2, 0), (1, 2), (-1, 2), (2, 1), (2, -1), (2, 2)]
STAGES = [[((0, 1), t), ((0, -1), t), ((1, 0), t + 2), ((-1, 0), t + 2)] for t in (0, 1)]
STAGES += [[((1, 0), t), ((-1, 0), t), ((0, 1), t + 2), ((0, -1), t + 2)] for t in (0, 1)]
CORNERS = [[((1, s), t), ((-1, s), t), ((s, 1), t + 2), ((s, -1), t + 2)] for t in (0, 1) for s in (1, -1)]
STAGES += CORNERS[:2] + [[((0, 2), 0), ((0, 2), 1), ((2, 0), 2), ((2, 0), 3)]] + CORNERS[2:]
STAGES += [[((a, b), 0), ((a, b), 1), ((b, a), 2), ((b, a), 3)] for a, b in PAIRS]
STAGE_OF = {piece: (k, j) for k, stage in enumerate(STAGES) for j, piece in enumerate(stage)}
STAGE_OF.update({((0, 0), t): (-1, t) for t in range(TILES)})
SHARE = (0.5, 0.5, 0.5, 0.5, 0.5, 0.5, 0.5, 0.5, 0.5, 0.5, 1.0, 0.0, 1.0, 0.0, 0.5)
RELAYS = {0: ((0, (0,)),), 1: ((1, (0,)), (0, (1,)), (1, (1,)))}
LOOPS = [
    [((1,), (0,)), ((2,), (1,)), ((3,), (2,)), ((6, 4), (3,)), ((5,), (6,))],
    [((7, 8), (4, 5)), ((9, 10, 11), (7, 8)), ((12, 13, 14), (9, 10)), ((), (12, 14)), ((), (11, 13))],
]


PLACE = {k: n for n, k in enumerate([-1] + [k for steps in LOOPS for _, computed in steps for k in computed])}


def wrap(d):
    return (d + 1) % SIDE - 1


def relays(piece):
    (slow, fast), t = piece
    swap = t >= TILES // 2
    if swap:
        slow, fast = fast, slow
    lead = 1 if t % 2 == 0 else -1
    hops = []
    if slow == 0 and fast == 0:
        hops += [(0, 1), (0, -1)]
    elif slow == 0 and fast == lead:
        hops += [(0, -fast)]
    if slow == 0:
        hops += [(1, 0), (-1, 0)]
    elif slow == lead:
        hops += [(-slow, 0)]
    return [(b, a) if swap else (a, b) for a, b in hops]


def relay_list(k, ranks=(0, 1)):
    pieces = [((0, 0), t) for t in range(TILES)] if k < 0 else STAGES[k]
    found = []
    for piece in pieces:
        swap = piece[1] >= TILES // 2
        for hop in relays(piece):
            along = hop[1] if not swap else hop[0]
            found.append((0 if along else 1, len(found), piece, hop))
    return [(piece, hop) for rank, _, piece, hop in sorted(found) if rank in ranks]


def merged(copies, join):
    found = []
    for piece, hop in copies:
        left = (piece[0], piece[1] - 1)
        beside = join and piece[1] % 2 == 1 and STAGE_OF[left][0] == STAGE_OF[piece][0]
        if beside and (left, 1, hop) in found:
            found[found.index((left, 1, hop))] = (left, 2, hop)
        else:
            found.append((piece, 1, hop))
    return found


def dot(lhs, rhs, dims):
    return lax.dot_general(lhs, rhs, (dims, ((), ())), preferred_element_type=F32)


def split3(val):
    hi = jnp.clip(val, -C_CAP, C_CAP).astype(BF16).astype(F32)
    mid = (val - hi).astype(BF16).astype(F32)
    low = (val - hi - mid).astype(BF16).astype(F32)
    return hi, mid, low


def kernel(width, x_ref, q_ref, cnt_ref, out_ref, e_ref, slots, xa, ci, s_acc, t_acc, e_acc, ebuf,
           send_sem, recv_sem, mate_sem, e_sem):
    rows = x_ref.shape[0]
    n_dev = 2 * SIDE * SIDE
    n_sends = sum(len(relay_list(k)) for k in range(-1, len(STAGES)))
    me = lax.axis_index('row')
    sys_id = lax.axis_index('sys')
    core = lax.rem(me, 2)
    chip = lax.div(me, 2)
    pos_y, pos_x = lax.div(chip, SIDE), lax.rem(chip, SIDE)
    mate = me + 1 - 2 * core
    scale = math.log2(math.e) / width

    def dev(dy, dx, plane):
        return (lax.rem(pos_y + dy + SIDE, SIDE) * SIDE + lax.rem(pos_x + dx + SIDE, SIDE)) * 2 + plane

    barrier = pltpu.get_barrier_semaphore()
    near = [dev(0, 1, core), dev(0, -1, core), dev(1, 0, core), dev(-1, 0, core), mate]
    for peer in near:
        pl.semaphore_signal(barrier, inc=1, device_id=(sys_id, peer), device_id_type=MESH)
    s_acc[...] = jnp.zeros_like(s_acc)
    t_acc[...] = jnp.zeros_like(t_acc)

    count = cnt_ref[0]
    row_id = lax.broadcasted_iota(jnp.int32, (rows, width), 0)
    lane_id = lax.broadcasted_iota(jnp.int32, (rows, width), 1)
    x_val = jnp.where(row_id < count, x_ref[...].astype(F32), 0.0)
    x_t = x_val.T
    s_row = -jnp.minimum(0.5 * jnp.sum(x_t * x_t, axis=0, keepdims=True), S_CAP)
    q_shape = q_ref.shape
    q_id = lax.broadcasted_iota(jnp.int32, q_shape, 0) * q_shape[1] + lax.broadcasted_iota(jnp.int32, q_shape, 1)
    q_val = jnp.where(q_id < count, q_ref[...], 0.0)
    q_row = jnp.concatenate([q_val[r:r + 1, :] for r in range(q_shape[0])], axis=1)
    aug_id = lax.broadcasted_iota(jnp.int32, (AUG, rows), 0)
    aug = jnp.where(aug_id < 3, 1.0, 0.0)
    for k, part in enumerate(split3(s_row) + split3(q_row)):
        aug = jnp.where(aug_id == 3 + k, part, aug)
    for t in range(TILES):
        cols = slice(t * TILE, (t + 1) * TILE)
        slots[t, :width, :] = x_t[:, cols].astype(BF16)
        slots[t, width:, :] = aug[:, cols].astype(BF16)
    pl.semaphore_wait(barrier, len(near))

    other = n_dev // 2 * TILES

    def unit_of(piece):
        k, j = STAGE_OF[piece]
        return PLACE[k] * TILES + j

    def remote(src, dst, tiles, send, recv, peer):
        return pltpu.make_async_remote_copy(
            src_ref=slots.at[pl.ds(src, tiles)], dst_ref=slots.at[pl.ds(dst, tiles)], send_sem=send, recv_sem=recv,
            device_id=(sys_id, peer), device_id_type=MESH)

    def start_relays(k, ranks):
        for piece, tiles, hop in merged(relay_list(k, ranks), k >= 0):
            there = ((wrap(piece[0][0] - hop[0]), wrap(piece[0][1] - hop[1])), piece[1])
            remote(unit_of(piece), unit_of(there), tiles, send_sem.at[0], recv_sem.at[STAGE_OF[there][0]],
                   dev(hop[0], hop[1], core)).start()

    def to_mate(k):
        first = PLACE[k] * TILES
        remote(first, other + first, TILES, send_sem.at[1], mate_sem.at[k + 1], mate).start()

    def arrive(k):
        remote(0, PLACE[k] * TILES, TILES, send_sem.at[0], recv_sem.at[k], mate).wait_recv()
        for stage, ranks in RELAYS.get(k, ((k, (0, 1)),)):
            start_relays(stage, ranks)
        to_mate(k)

    def from_mate(k):
        remote(0, other + PLACE[k] * TILES, TILES, send_sem.at[1], mate_sem.at[k + 1], mate).wait_recv()

    start_relays(-1, (0, 1))
    to_mate(-1)

    s_col = -jnp.minimum(0.5 * jnp.sum(x_val * x_val, axis=1, keepdims=True), S_CAP)
    xa[:, :width] = x_val.astype(BF16)
    tail = jnp.where((lane_id >= 3) & (lane_id < 6), 1.0, 0.0)
    for k, part in enumerate(split3(s_col)):
        tail = jnp.where(lane_id == k, part, tail)
    xa[:, width:] = tail.astype(BF16)
    q_t = q_val.T
    for r in range(q_shape[0]):
        lanes = q_shape[1]
        ci[r * lanes:(r + 1) * lanes, :] = jnp.broadcast_to(q_t[:, r:r + 1], (lanes, width))

    eye = (lax.broadcasted_iota(jnp.int32, (TILE, TILE), 0) == lax.broadcasted_iota(jnp.int32, (TILE, TILE), 1))
    pad = jnp.zeros((width - AUG, TILE), BF16)

    def column_tile(unit, diag=None):
        block = slots[unit]
        rhs = jnp.concatenate([block, pad], axis=0)
        parts = block[width:, :].astype(F32)
        c_cols = parts[6:7, :] + parts[7:8, :] + parts[8:9, :]
        high = TILE if diag is not None else 2 * TILE
        for it in range(rows // high):
            mine = slice(it * high, (it + 1) * high)
            arg = dot(xa[mine, :], rhs, ((1,), (0,)))
            weight = jnp.exp2(jnp.minimum(arg, 0.0) * scale) * c_cols
            if diag is not None and it == diag:
                weight = jnp.where(eye, 0.0, weight)
            c_mine = ci[mine, :]
            left, right = weight[:, :width] * c_mine, weight[:, width:] * c_mine
            s_acc[mine, :] += left + right
            w_low = jnp.concatenate([left, right], axis=1).astype(BF16)
            t_acc[mine, :] += dot(w_low, block[:width, :], ((1,), (1,)))

    for t in range(TILES):
        column_tile(t, diag=t)
    from_mate(-1)
    for t in range(TILES):
        column_tile(other + t)
    e_acc[...] = jnp.zeros_like(e_acc)
    arrive(0)
    for t in range(TILES):
        column_tile(TILES + t)

    early = LOOPS[0]
    assert all(SHARE[k] == 0.5 for _, computed in early for k in computed)

    def early_body(step, carry):
        for now, (arriving, computed) in enumerate(early[:-1]):
            @pl.when(step == now)
            def _():
                for k in arriving:
                    arrive(k)
                from_mate(computed[0])
        for j in range(TILES):
            column_tile(other + (step + 1) * TILES + j)
            column_tile((step + 2) * TILES + j)
        return carry
    lax.fori_loop(0, len(early) - 1, early_body, 0)
    for k in early[-1][0]:
        arrive(k)
    from_mate(early[-1][1][0])
    for j in range(TILES):
        column_tile(other + len(early) * TILES + j)

    def e_copy(first, count, peer):
        ref = ebuf.at[pl.ds(first, count)]
        return pltpu.make_async_remote_copy(src_ref=ref, dst_ref=ref, send_sem=e_sem.at[0], recv_sem=e_sem.at[1],
                                            device_id=(sys_id, peer), device_id_type=MESH)

    def e_start(step, carry):
        e_copy(me, 1, lax.rem(me + step, n_dev)).start()
        return carry

    def tally(weight):
        e_acc[...] += weight * jnp.sum(s_acc[...].reshape(rows // 8, 8, width), axis=0)

    def run_loop(steps, share, share_after):
        shares = [share] + [SHARE[computed[-1]] for _, computed in steps]
        starts = [SHARE[computed[0]] for _, computed in steps]
        inner = [SHARE[computed[0]] - SHARE[computed[-1]] for _, computed in steps]

        def step_body(step, carry):
            for now, (arriving, computed) in enumerate(steps):
                @pl.when(step == now)
                def _():
                    for k in arriving:
                        arrive(k)
                    for k in computed:
                        from_mate(k)
                    if shares[now] != starts[now]:
                        tally(shares[now] - starts[now])
                    if share_after is None and now == len(steps) - 1:
                        assert not any(SHARE[k] for k in computed)
                        ebuf[me] = e_acc[...]
                        lax.fori_loop(1, n_dev, e_start, 0)
            for i in range(len(steps[0][1])):
                if i and any(inner):
                    weight = jnp.float32(0.0)
                    for now, change in enumerate(inner):
                        weight = jnp.where(step == now, change, weight)
                    tally(weight)
                first = (PLACE[steps[0][1][0]] + step * len(steps[0][1]) + i) * TILES
                for j in range(TILES):
                    column_tile(first + j)
                    column_tile(other + first + j)
            return carry
        lax.fori_loop(0, len(steps), step_body, 0)
        return shares[-1]

    run_loop(LOOPS[1], 0.5, None)

    s_sum = jnp.sum(s_acc[...], axis=1, keepdims=True)
    out_ref[...] = (s_sum * xa[:, :width].astype(F32) - t_acc[...]) * (1.0 / width)

    e_copy(0, n_dev - 1, mate).wait_recv()
    e_ref[0] = jnp.sum(ebuf[...])
    e_copy(0, n_dev - 1, mate).wait_send()
    remote(0, 0, n_sends, send_sem.at[0], recv_sem.at[0], mate).wait_send()
    remote(0, 0, other, send_sem.at[1], mate_sem.at[0], mate).wait_send()


def solution(mesh):
    n_dev = mesh.shape['row']
    assert n_dev == 2 * SIDE * SIDE

    def per_device(positions, charges, counts):
        rows, width = positions.shape
        assert rows == TILE * TILES and 2 * width == TILE
        vmem = pl.BlockSpec(memory_space=pltpu.VMEM)
        smem = pl.BlockSpec(memory_space=pltpu.SMEM)
        force, energy = pl.pallas_call(
            functools.partial(kernel, width),
            out_shape=[jax.ShapeDtypeStruct((rows, width), F32), jax.ShapeDtypeStruct((1,), F32)],
            in_specs=[vmem, vmem, smem],
            out_specs=[pl.BlockSpec(memory_space=pltpu.VMEM), smem],
            scratch_shapes=[
                pltpu.VMEM((n_dev * TILES, width + AUG, TILE), BF16),
                pltpu.VMEM((rows, 2 * width), BF16),
                pltpu.VMEM((rows, width), F32),
                pltpu.VMEM((rows, width), F32),
                pltpu.VMEM((rows, width), F32),
                pltpu.VMEM((8, width), F32),
                pltpu.VMEM((n_dev, 8, width), F32),
                pltpu.SemaphoreType.DMA((2,)),
                pltpu.SemaphoreType.DMA((len(STAGES),)),
                pltpu.SemaphoreType.DMA((len(STAGES) + 1,)),
                pltpu.SemaphoreType.DMA((2,)),
            ],
            compiler_params=pltpu.CompilerParams(collective_id=0, has_side_effects=True, vmem_limit_bytes=48 * 2 ** 20),
            name='pair_forces',
        )(positions, charges.reshape(rows // width, width), counts)
        return force, energy

    row_spec = P(('sys', 'row'), None)
    vec_spec = P(('sys', 'row'))
    return jax.shard_map(per_device, mesh=mesh, in_specs=(row_spec, vec_spec, vec_spec),
                         out_specs=(row_spec, P('sys')), check_vma=False)
```
